256 devices in a mesh: rows: 32 (over x, z), grp: 8 (over y, core).
Axes of the slice: x: 4, y: 4, z: 8, core: 2. Of those that a mesh axis runs over, the one named last changes fastest.
Arguments:
- sketch: float32 [2048, 65536], P(None, ('rows', 'grp')), may hold values from -0.125 to 0.125
- prior_basis: float32 [65536, 512], P(('rows', 'grp'))
- panel_block: float32 [65536, 256], P(('rows', 'grp'))
- panel_index: int32 [1], replicated, may hold values from 0 to 2
- prior_count: int32 [1], replicated, may hold values from 384 to 512
Outputs:
- new_basis: float32 [65536, 128], P(('rows', 'grp'))
- factors: float32 [640, 128], replicated
The draws below stay inside these ranges and needn't reach their ends.
All inputs are finite; a program needn't handle non-finite values.
Results may differ from the reference program's by a relative error of at most 0.00011.
Values sent between devices are 32-bit elements; how exact they have to be, the bound alone decides.
A program may use at most 64 MiB of HBM per device.

```python
import jax
import jax.numpy as jnp
from jax import lax

SK = 2048
NP = 512
P_SIZE = 64
BLOCK_PANELS = 4
ROWS = 65536


def draw_both(key):
    base = jax.random.fold_in(key, 11)
    first_key, second_key, third_key = jax.random.split(base, 3)
    place = jnp.arange(ROWS, dtype=jnp.float32) / max(ROWS - 1, 1)
    scales = 3.0 ** place
    basis = jax.random.normal(first_key, (ROWS, NP), jnp.float32)
    noise = jax.random.normal(third_key, (ROWS, BLOCK_PANELS * P_SIZE), jnp.float32)
    basis = basis * scales[:, None] * ROWS ** (-0.5)
    mixing = jax.random.normal(second_key, (NP, BLOCK_PANELS * P_SIZE), jnp.float32)
    panels = jnp.dot(basis, mixing) + 4.0 * ROWS ** (-0.5) * noise * scales[:, None]
    return (basis, panels)


def draw_prior_basis(key, part):
    return draw_both(key)[0]


def draw_panel_block(key, part):
    return draw_both(key)[1]


def steps_of(stream_key, dims, cuts, low, high):
    factor_of = 1.0
    for axis_at, parts in cuts:
        draws = jax.random.uniform(jax.random.fold_in(jax.random.fold_in(stream_key, 6), axis_at), (parts,), jnp.float32, low / len(cuts), high / len(cuts))
        factor_of = factor_of * jnp.repeat(jnp.exp(draws), dims[axis_at] // parts).reshape((-1,) + (1,) * (len(dims) - 1 - axis_at))
    return factor_of


def gaussian(key, dims, spread, reach, cuts=(), kind=jnp.bfloat16):
    loudness = steps_of(key, dims, cuts, -0.22, 0.18) if cuts else 1.0
    array = jax.random.normal(key, dims, jnp.float32) * spread * loudness
    return jnp.minimum(jnp.maximum(array, -reach), reach).astype(kind)


def setup_inputs(seed: int = 0) -> dict:
    splits = jax.random.split(jax.random.key(seed), 6)
    sketch = gaussian(splits[0], (SK, ROWS), SK ** -0.5, 0.125, ((1, 256),), jnp.float32)
    prior_basis = draw_prior_basis(jax.random.fold_in(splits[5], 71), 0)
    panel_block = draw_panel_block(jax.random.fold_in(splits[5], 71), 0)
    panel_index = jax.random.randint(splits[3], (1,), 0, BLOCK_PANELS - 1).astype(jnp.int32)
    prior_count = jax.random.randint(splits[4], (1,), NP - 2 * P_SIZE, NP + 1).astype(jnp.int32)
    return {"sketch": sketch, "prior_basis": prior_basis, "panel_block": panel_block, "panel_index": panel_index, "prior_count": prior_count}


def matmul(left, right):
    return jnp.dot(left, right, precision=lax.Precision.HIGHEST)

def right_solve(factor, values):
    return jax.scipy.linalg.solve_triangular(factor, values.T, lower=True).T

def reference(sketch, prior_basis, panel_block, panel_index, prior_count):
    width = prior_basis.shape[1]
    column_keep = (jnp.arange(width) < prior_count[0]).astype(jnp.float32)
    masked = prior_basis * column_keep
    start = (panel_index[0] * P_SIZE).astype(jnp.int32)
    chosen = lax.dynamic_slice_in_dim(panel_block, start, 2 * P_SIZE, 1)
    first = chosen[:, :P_SIZE]
    second = chosen[:, P_SIZE:]
    prior_sketch = matmul(sketch, masked)
    sketch_one = matmul(sketch, first)
    sketch_two = matmul(sketch, second)
    gram_prior = matmul(prior_sketch.T, prior_sketch) + jnp.diag(1.0 - column_keep)
    prior_factor = jnp.linalg.cholesky(gram_prior)
    coef_one = jax.scipy.linalg.cho_solve((prior_factor, True), matmul(prior_sketch.T, sketch_one))
    resid_one = first - matmul(masked, coef_one)
    skres_one = sketch_one - matmul(prior_sketch, coef_one)
    tri_one = jnp.linalg.cholesky(matmul(resid_one.T, resid_one))
    basis_one = right_solve(tri_one, resid_one)
    skbasis_one = right_solve(tri_one, skres_one)
    coef_two = jax.scipy.linalg.cho_solve((prior_factor, True), matmul(prior_sketch.T, sketch_two))
    resid_two = second - matmul(masked, coef_two)
    skres_two = sketch_two - matmul(prior_sketch, coef_two)
    small_factor = jnp.linalg.cholesky(matmul(skbasis_one.T, skbasis_one))
    inner = jax.scipy.linalg.cho_solve((small_factor, True), matmul(skbasis_one.T, skres_two))
    final_two = resid_two - matmul(basis_one, inner)
    tri_two = jnp.linalg.cholesky(matmul(final_two.T, final_two))
    basis_two = right_solve(tri_two, final_two)
    scale_rows = jnp.sqrt(jnp.float32(prior_basis.shape[0]))
    new_basis = jnp.concatenate([basis_one, basis_two], axis=1) * scale_rows
    upper = jnp.concatenate([tri_one.T, inner], axis=1)
    lower_rows = jnp.concatenate([jnp.zeros((P_SIZE, P_SIZE), jnp.float32), tri_two.T], axis=1)
    factors = jnp.concatenate([jnp.concatenate([coef_one, coef_two], axis=1), upper, lower_rows], axis=0)
    return (new_basis, factors)
```

```python
import jax
import jax.numpy as jnp
from jax import lax
from jax.experimental import pallas as pl
from jax.experimental.pallas import tpu as pltpu
from jax.sharding import Mesh
from jax.sharding import PartitionSpec as P

P_SIZE = 64
AXES = ("x", "z", "y", "c")
MESH = pl.DeviceIdType.MESH
F32 = jnp.float32
BF16 = jnp.bfloat16


def vmem():
    return pl.BlockSpec(memory_space=pltpu.VMEM)


def dot(left, right):
    return jnp.dot(left, right, precision=lax.Precision.HIGHEST, preferred_element_type=F32)


def dot_rows(left, right):
    return lax.dot_general(
        left, right, (((0,), (0,)), ((), ())), precision=lax.Precision.HIGHEST, preferred_element_type=F32
    )


def split(value):
    high = value.astype(BF16)
    return high, (value - high.astype(F32)).astype(BF16)


def halves(place):
    first = (place + 1) - 2 * lax.rem(place, 2)
    second = lax.rem(place + 3 + 2 * lax.rem(place, 2), 4)
    return (first, lax.rem((place + 1) // 2, 2)), (second, place // 2)


def gram_kernel(sketch, wide, out, high, low, away, came, acc, r0, r1, r2, r3, zout, zin, zall, full, mine, other,
                d_send, d_recv, r_send, r_recv, z_send, z_recv, y_send, y_recv, a_send, a_recv, m_send, m_recv):
    x, z, y, c = (lax.axis_index(name) for name in AXES)
    (xa, xa_bit), (xb, xb_bit) = halves(x)
    (ya, ya_bit), (yb, yb_bit) = halves(y)
    links = (({"x": xa}, xa_bit), ({"y": ya}, ya_bit), ({"x": xb}, xb_bit), ({"y": yb}, yb_bit))
    ring = [{"z": lax.rem(z + step, 8)} for step in range(1, 8)]
    peer = {"c": 1 - c}

    barrier = pltpu.get_barrier_semaphore()
    for target in [peer] + [link for link, _ in links] + ring:
        pl.semaphore_signal(barrier, inc=1, device_id=target, device_id_type=MESH)

    def remote(source, target, send, recv, device):
        return pltpu.make_async_remote_copy(
            src_ref=source, dst_ref=target, send_sem=send, recv_sem=recv, device_id=device, device_id_type=MESH
        )

    starts, sent = [], []
    for s in range(4):
        at, kept, gone = 0, [0], []
        for t in range(4):
            size = 16 >> t
            bit = links[(s + t) % 4][1]
            gone.append(at + (1 - bit) * size)
            at = at + bit * size
            kept.append(at)
        starts.append(kept)
        sent.append(gone)

    wide_high, wide_low = split(wide[...])
    high[...] = wide_high
    low[...] = wide_low

    def product(row):
        part_high, part_low = split(sketch[pl.ds(pl.multiple_of(row, 128), 128), :])
        value = jnp.dot(part_high, low[...], preferred_element_type=F32)
        value = value + jnp.dot(part_low, high[...], preferred_element_type=F32)
        return value + jnp.dot(part_high, high[...], preferred_element_type=F32)

    def spot(i):
        s, kept = lax.rem(i, 4), i // 4
        bit = lax.rem(s, 2) * (ya_bit * (1 - s // 2) + yb_bit * (s // 2))
        bit = bit + (1 - lax.rem(s, 2)) * (xa_bit * (1 - s // 2) + xb_bit * (s // 2))
        return s, 16 * (kept * bit + (1 - kept) * (1 - bit))

    def chunk(i):
        s, tile = spot(i)
        return remote(away.at[s, pl.ds(tile, 16)], came.at[s, pl.ds(tile, 16)], d_send.at[i], d_recv.at[i], peer)

    def for_peer(i, carry):
        s, tile = spot(i)
        away[s, pl.ds(tile, 16)] = product((1 - c) * 1024 + s * 256 + tile * 8).reshape(16, 8, 640)

        @pl.when(i == 0)
        def _():
            pl.semaphore_wait(barrier, 12)

        chunk(i).start()
        return carry

    def for_self(i, carry):
        s, tile = spot(i)
        acc[s, pl.ds(tile, 16)] = product(c * 1024 + s * 256 + tile * 8).reshape(16, 8, 640)
        return carry

    lax.fori_loop(0, 8, for_peer, 0)
    lax.fori_loop(0, 8, for_self, 0)

    landing = (r0, r1, r2, r3)

    def scatter(t, s):
        size = 16 >> t
        return remote(
            acc.at[s, pl.ds(sent[s][t], size)], landing[t].at[s], r_send.at[t, s], r_recv.at[t, s],
            links[(s + t) % 4][0],
        )

    for i in range(8):
        s, tile = spot(i)
        chunk(i).wait_recv()
        acc[s, pl.ds(tile, 16)] += came[s, pl.ds(tile, 16)]
        if i < 4:
            scatter(0, i).start()
    for t in range(4):
        size = 16 >> t
        for s in range(4):
            scatter(t, s).wait_recv()
            at = starts[s][t + 1]
            if t < 3:
                acc[s, pl.ds(at, size)] += landing[t][s]
                scatter(t + 1, s).start()
            else:
                zout[pl.ds(2 * s, 2)] = acc[s, pl.ds(at, 2)] + r3[s]

    def along(step):
        return remote(
            zout.at[lax.rem(z + step, 8)], zin.at[step - 1], z_send.at[step - 1], z_recv.at[step - 1], ring[step - 1]
        )

    def back(step):
        return remote(zall.at[z], zall.at[z], y_send.at[step - 1], y_recv.at[step - 1], ring[step - 1])

    for step in range(1, 8):
        along(step).start()
    total = zout[z]
    for step in range(1, 8):
        along(step).wait_recv()
        total = total + zin[step - 1]
    zall[z] = total
    for step in range(1, 8):
        back(step).start()
    for step in range(1, 8):
        back(step).wait_recv()

    def gather(t, s):
        size = 16 >> t
        here = full.at[s, pl.ds(starts[s][t + 1], size)]
        source = zall.at[pl.ds(2 * s, 2)] if t == 3 else here
        return remote(source, here, a_send.at[t, s], a_recv.at[t, s], links[(s + t) % 4][0])

    for s in range(4):
        gather(3, s).start()
    for s in range(4):
        full[s, pl.ds(starts[s][4], 2)] = zall[pl.ds(2 * s, 2)]
    for t in (2, 1, 0):
        for s in range(4):
            gather(t + 1, s).wait_recv()
            gather(t, s).start()

    def add_gram(rows, first):
        part_high, part_low = split(rows)
        for i in range(5):
            lo = 128 * i
            value = None
            for left in (part_low, part_high):
                for right in (part_low, part_high):
                    term = lax.dot_general(
                        left[:, lo:lo + 128], right[:, lo:], (((0,), (0,)), ((), ())), preferred_element_type=F32
                    )
                    value = term if value is None else value + term
            if first:
                mine[lo:lo + 128, lo:] = value
            else:
                mine[lo:lo + 128, lo:] += value

    add_gram(jnp.concatenate([full[s, pl.ds(starts[s][1], 16)].reshape(128, 640) for s in range(4)], axis=0), True)
    for s in (0, 2):
        rows = []
        for u in (s, s + 1):
            gather(0, u).wait_recv()
            rows.append(full[u, pl.ds(sent[u][0], 16)].reshape(128, 640))
        add_gram(jnp.concatenate(rows, axis=0), False)

    def swap(i):
        lo = 128 * i
        return remote(
            mine.at[pl.ds(lo, 128), pl.ds(lo, 640 - lo)], other.at[pl.ds(lo, 128), pl.ds(lo, 640 - lo)],
            m_send.at[i], m_recv.at[i], peer,
        )

    for i in range(5):
        swap(i).start()
    for i in range(5):
        lo = 128 * i
        swap(i).wait_recv()
        out[lo:lo + 128, lo:] = mine[lo:lo + 128, lo:] + other[lo:lo + 128, lo:]
        if i:
            out[lo:lo + 128, :lo] = jnp.zeros((128, lo), F32)

    for i in range(8):
        chunk(i).wait_send()
    for t in range(4):
        for s in range(4):
            scatter(t, s).wait_send()
            gather(t, s).wait_send()
    for step in range(1, 8):
        along(step).wait_send()
        back(step).wait_send()
    for i in range(5):
        swap(i).wait_send()


def sketch_gram(sketch, wide):
    dma = pltpu.SemaphoreType.DMA
    scratch = [pltpu.VMEM((256, 640), BF16)] * 2
    scratch += [pltpu.VMEM((4, 32, 8, 640), F32)] * 3
    scratch += [pltpu.VMEM((4, 16 >> t, 8, 640), F32) for t in range(4)]
    scratch += [pltpu.VMEM((8, 8, 640), F32), pltpu.VMEM((7, 8, 640), F32), pltpu.VMEM((8, 8, 640), F32)]
    scratch += [pltpu.VMEM((4, 32, 8, 640), F32)]
    scratch += [pltpu.VMEM((640, 640), F32)] * 2
    scratch += [dma((8,))] * 2 + [dma((4, 4))] * 2 + [dma((7,))] * 4 + [dma((4, 4))] * 2 + [dma((5,))] * 2
    return pl.pallas_call(
        gram_kernel,
        out_shape=jax.ShapeDtypeStruct((640, 640), F32),
        in_specs=[vmem()] * 2,
        out_specs=vmem(),
        scratch_shapes=scratch,
        compiler_params=pltpu.CompilerParams(
            collective_id=0, has_side_effects=True, vmem_limit_bytes=48 * 1024 * 1024
        ),
        name="sketch_gram",
    )(sketch, wide)


def sweep(blocks, panels):
    blocks = list(blocks)
    lane = lax.broadcasted_iota(jnp.int32, (8, 128), 1)
    row = lax.broadcasted_iota(jnp.int32, (8, 128), 0)
    for p in range(panels):
        k = 8 * p
        inside = (lane >= k) & (lane < k + 8)
        cols = [[jnp.broadcast_to(b[:, k + s:k + s + 1], (8, 128)) for s in range(8)] for b in blocks]
        e = list(cols[p])
        r = jnp.where(inside, (lane - k == row).astype(F32), blocks[p])
        for s in range(8):
            inv = 1.0 / e[s][s:s + 1, :]
            rs = r[s:s + 1, :] * inv
            r = jnp.where(row == s, rs, r - e[s] * rs)
            for u in range(s + 1, 8):
                es = e[u][s:s + 1, :] * inv
                e[u] = jnp.where(row == s, es, e[u] - e[s] * es)
        rows = [r[s:s + 1, :] for s in range(8)]
        for i in range(len(blocks)):
            if i == p:
                continue
            total = jnp.where(inside, 0.0, blocks[i])
            for s in range(8):
                total = total - cols[i][s] * rows[s]
            blocks[i] = total
        blocks[p] = r
    return blocks


def solve_kernel(count, gram, wide, coef, resid, small, a):
    r = lax.broadcasted_iota(jnp.int32, (128, 128), 0)
    c = lax.broadcasted_iota(jnp.int32, (128, 128), 1)
    a[...] = gram[...]
    for k in range(4):
        lo = 128 * k
        hi = lo + 128
        unused = (c + lo >= count[0]) & (r == c)
        block = a[lo:hi, lo:hi] + jnp.where(unused, 1.0, 0.0)
        inverse = jnp.concatenate(sweep([block[8 * i:8 * i + 8] for i in range(16)], 16), axis=0)
        y = dot(inverse, a[lo:hi, hi:])
        for i in range(k + 1, 5):
            left = 128 * i
            a[left:left + 128, left:] -= dot_rows(a[lo:hi, left:left + 128], y[:, left - hi:])
        if k:
            a[:lo, hi:] -= dot(a[:lo, lo:hi], y)
        a[lo:hi, hi:] = y
    coefs = a[:512, 512:]
    tail = a[512:, 512:]
    both = jnp.concatenate(sweep([tail[8 * i:8 * i + 8] for i in range(8)], 8), axis=0)
    ratio = both[:, P_SIZE:]
    coef[0:512, :] = coefs
    coef[512:576, :] = both
    left = wide[:, 512:] - dot(wide[:, :512], coefs)
    first = left[:, :P_SIZE]
    second = left[:, P_SIZE:] - dot(first, ratio)
    final = jnp.concatenate([first, second], axis=1)
    resid[...] = final
    own = dot_rows(final, final)
    small[...] = jnp.concatenate([own[:P_SIZE, :P_SIZE], own[P_SIZE:, P_SIZE:]], axis=1)


def solve(count, gram, wide):
    return pl.pallas_call(
        solve_kernel,
        out_shape=(
            jax.ShapeDtypeStruct((576, 128), F32),
            jax.ShapeDtypeStruct((256, 128), F32),
            jax.ShapeDtypeStruct((64, 128), F32),
        ),
        in_specs=[pl.BlockSpec(memory_space=pltpu.SMEM), vmem(), vmem()],
        out_specs=(vmem(),) * 3,
        scratch_shapes=[pltpu.VMEM((640, 640), F32)],
        compiler_params=pltpu.CompilerParams(vmem_limit_bytes=32 * 1024 * 1024),
        name="solve",
    )(count, gram, wide)


def sum_kernel(small, out, peer_in, half, x_in, xy, y_in, xyz, z_in, done,
               p_send, p_recv, x_send, x_recv, y_send, y_recv, z_send, z_recv, b_send, b_recv):
    x, z, y, c = (lax.axis_index(name) for name in AXES)
    peer = {"c": 1 - c}
    xs = [{"x": lax.rem(x + step, 4)} for step in range(1, 4)]
    ys = [{"y": lax.rem(y + step, 4)} for step in range(1, 4)]
    zs = [{"z": lax.rem(z + step, 8)} for step in range(1, 8)]
    barrier = pltpu.get_barrier_semaphore()
    for target in [peer] + xs + ys + zs:
        pl.semaphore_signal(barrier, inc=1, device_id=target, device_id_type=MESH)
    pl.semaphore_wait(barrier, 14)

    def remote(source, target, send, recv, device):
        return pltpu.make_async_remote_copy(
            src_ref=source, dst_ref=target, send_sem=send, recv_sem=recv, device_id=device, device_id_type=MESH
        )

    def exchange(source, target, send, recv, devices):
        return [remote(source, target.at[i], send.at[i], recv.at[i], device) for i, device in enumerate(devices)]

    theirs = pl.ds(pl.multiple_of(32 * (1 - c), 32), 32)
    ours = pl.ds(pl.multiple_of(32 * c, 32), 32)
    across = remote(small.at[theirs], peer_in, p_send, p_recv, peer)
    across.start()
    across.wait_recv()
    half[...] = small[ours, :] + peer_in[...]
    on_x = exchange(half, x_in, x_send, x_recv, xs)
    for copy in on_x:
        copy.start()
    for copy in on_x:
        copy.wait_recv()
    xy[...] = half[...] + x_in[0] + x_in[1] + x_in[2]
    on_y = exchange(xy, y_in, y_send, y_recv, ys)
    for copy in on_y:
        copy.start()
    for copy in on_y:
        copy.wait_recv()
    xyz[...] = xy[...] + y_in[0] + y_in[1] + y_in[2]
    on_z = exchange(xyz, z_in, z_send, z_recv, zs)
    for copy in on_z:
        copy.start()
    total = xyz[...]
    for copy in on_z:
        copy.wait_recv()
    for i in range(7):
        total = total + z_in[i]
    done[...] = total
    out[ours, :] = total
    back = remote(done, out.at[ours], b_send, b_recv, peer)
    back.start()
    back.wait_recv()
    for copy in [across, back] + on_x + on_y + on_z:
        copy.wait_send()


def sum_small(small):
    dma = pltpu.SemaphoreType.DMA
    block = (32, 128)
    return pl.pallas_call(
        sum_kernel,
        out_shape=jax.ShapeDtypeStruct((64, 128), F32),
        in_specs=[vmem()],
        out_specs=vmem(),
        scratch_shapes=[
            pltpu.VMEM(block, F32), pltpu.VMEM(block, F32), pltpu.VMEM((3,) + block, F32), pltpu.VMEM(block, F32),
            pltpu.VMEM((3,) + block, F32), pltpu.VMEM(block, F32), pltpu.VMEM((7,) + block, F32), pltpu.VMEM(block, F32),
            dma, dma, dma((3,)), dma((3,)), dma((3,)), dma((3,)), dma((7,)), dma((7,)), dma, dma,
        ],
        compiler_params=pltpu.CompilerParams(collective_id=1, has_side_effects=True),
        name="sum_small",
    )(small)


def shards(sketch, prior_basis, panel_block, panel_index, prior_count):
    width = prior_basis.shape[1]
    column_keep = (jnp.arange(width) < prior_count[0]).astype(F32)
    chosen = lax.dynamic_slice_in_dim(panel_block, panel_index[0] * P_SIZE, 2 * P_SIZE, 1)
    wide = jnp.concatenate([prior_basis * column_keep, chosen], axis=1)
    gram = sketch_gram(sketch, wide)
    coef, resid, small = solve(prior_count, gram, wide)
    grams = sum_small(small)
    total_rows = prior_basis.shape[0] * 256
    scale_rows = jnp.sqrt(jnp.float32(total_rows))
    tri_one = jnp.linalg.cholesky(grams[:, :P_SIZE])
    tri_two = jnp.linalg.cholesky(grams[:, P_SIZE:])
    basis_one = jax.scipy.linalg.solve_triangular(tri_one, resid[:, :P_SIZE].T, lower=True).T
    basis_two = jax.scipy.linalg.solve_triangular(tri_two, resid[:, P_SIZE:].T, lower=True).T
    inner = jnp.dot(tri_one.T, coef[512:, P_SIZE:], precision=lax.Precision.HIGHEST)
    new_basis = jnp.concatenate([basis_one, basis_two], axis=1) * scale_rows
    upper = jnp.concatenate([tri_one.T, inner], axis=1)
    lower = jnp.concatenate([jnp.zeros((P_SIZE, P_SIZE), F32), tri_two.T], axis=1)
    return new_basis, jnp.concatenate([coef[:512], upper, lower], axis=0)


def solution(mesh):
    torus = Mesh(mesh.devices.reshape(4, 8, 4, 2), AXES)
    return jax.shard_map(
        shards,
        mesh=torus,
        in_specs=(P(None, AXES), P(AXES, None), P(AXES, None), P(), P()),
        out_specs=(P(AXES, None), P()),
        check_vma=False,
    )
```

```python
import functools
import math

import jax
import jax.numpy as jnp
from jax import lax
from jax.experimental import pallas as pl
from jax.experimental.pallas import tpu as pltpu
from jax.sharding import Mesh
from jax.sharding import PartitionSpec as P

P_SIZE = 64
AXES = ("x", "z", "y", "c")
MESH = pl.DeviceIdType.MESH
F32 = jnp.float32
BF16 = jnp.bfloat16


def vmem():
    return pl.BlockSpec(memory_space=pltpu.VMEM)


def dot(left, right):
    return jnp.dot(left, right, precision=lax.Precision.HIGHEST, preferred_element_type=F32)


def dot_rows(left, right):
    return lax.dot_general(
        left, right, (((0,), (0,)), ((), ())), precision=lax.Precision.HIGHEST, preferred_element_type=F32
    )


def split(value):
    high = value.astype(BF16)
    return high, (value - high.astype(F32)).astype(BF16)


def halves(place):
    first = (place + 1) - 2 * lax.rem(place, 2)
    second = lax.rem(place + 3 + 2 * lax.rem(place, 2), 4)
    return (first, lax.rem((place + 1) // 2, 2)), (second, place // 2)


def gram_kernel(sketch, wide, out, high, low, away, came, acc, r0, r1, r2, r3, zout, zin, zall, full, mine, other,
                d_send, d_recv, r_send, r_recv, z_send, z_recv, y_send, y_recv, a_send, a_recv, m_send, m_recv):
    x, z, y, c = (lax.axis_index(name) for name in AXES)
    (xa, xa_bit), (xb, xb_bit) = halves(x)
    (ya, ya_bit), (yb, yb_bit) = halves(y)
    links = (({"x": xa}, xa_bit), ({"y": ya}, ya_bit), ({"x": xb}, xb_bit), ({"y": yb}, yb_bit))
    ring = [{"z": lax.rem(z + step, 8)} for step in range(1, 8)]
    peer = {"c": 1 - c}

    barrier = pltpu.get_barrier_semaphore()
    for target in [peer] + [link for link, _ in links] + ring:
        pl.semaphore_signal(barrier, inc=1, device_id=target, device_id_type=MESH)

    def remote(source, target, send, recv, device):
        return pltpu.make_async_remote_copy(
            src_ref=source, dst_ref=target, send_sem=send, recv_sem=recv, device_id=device, device_id_type=MESH
        )

    starts, sent = [], []
    for s in range(4):
        at, kept, gone = 0, [0], []
        for t in range(4):
            size = 16 >> t
            bit = links[(s + t) % 4][1]
            gone.append(at + (1 - bit) * size)
            at = at + bit * size
            kept.append(at)
        starts.append(kept)
        sent.append(gone)

    wide_high, wide_low = split(wide[...])
    high[...] = wide_high
    low[...] = wide_low

    def product(row):
        part_high, part_low = split(sketch[pl.ds(pl.multiple_of(row, 128), 128), :])
        value = jnp.dot(part_high, low[...], preferred_element_type=F32)
        value = value + jnp.dot(part_low, high[...], preferred_element_type=F32)
        return value + jnp.dot(part_high, high[...], preferred_element_type=F32)

    def spot(i):
        s, kept = lax.rem(i, 4), i // 4
        bit = lax.rem(s, 2) * (ya_bit * (1 - s // 2) + yb_bit * (s // 2))
        bit = bit + (1 - lax.rem(s, 2)) * (xa_bit * (1 - s // 2) + xb_bit * (s // 2))
        return s, 16 * (kept * bit + (1 - kept) * (1 - bit))

    def chunk(i):
        s, tile = spot(i)
        return remote(away.at[s, pl.ds(tile, 16)], came.at[s, pl.ds(tile, 16)], d_send.at[i], d_recv.at[i], peer)

    def for_peer(i, carry):
        s, tile = spot(i)
        away[s, pl.ds(tile, 16)] = product((1 - c) * 1024 + s * 256 + tile * 8).reshape(16, 8, 640)

        @pl.when(i == 0)
        def _():
            pl.semaphore_wait(barrier, 12)

        chunk(i).start()
        return carry

    def for_self(i, carry):
        s, tile = spot(i)
        acc[s, pl.ds(tile, 16)] = product(c * 1024 + s * 256 + tile * 8).reshape(16, 8, 640)
        return carry

    lax.fori_loop(0, 8, for_peer, 0)
    lax.fori_loop(0, 8, for_self, 0)

    landing = (r0, r1, r2, r3)

    def scatter(t, s):
        size = 16 >> t
        return remote(
            acc.at[s, pl.ds(sent[s][t], size)], landing[t].at[s], r_send.at[t, s], r_recv.at[t, s],
            links[(s + t) % 4][0],
        )

    for i in range(8):
        s, tile = spot(i)
        chunk(i).wait_recv()
        acc[s, pl.ds(tile, 16)] += came[s, pl.ds(tile, 16)]
        if i < 4:
            scatter(0, i).start()
    for t in range(4):
        size = 16 >> t
        for s in range(4):
            scatter(t, s).wait_recv()
            at = starts[s][t + 1]
            if t < 3:
                acc[s, pl.ds(at, size)] += landing[t][s]
                scatter(t + 1, s).start()
            else:
                zout[pl.ds(2 * s, 2)] = acc[s, pl.ds(at, 2)] + r3[s]

    def along(step):
        return remote(
            zout.at[lax.rem(z + step, 8)], zin.at[step - 1], z_send.at[step - 1], z_recv.at[step - 1], ring[step - 1]
        )

    def back(step):
        return remote(zall.at[z], zall.at[z], y_send.at[step - 1], y_recv.at[step - 1], ring[step - 1])

    for step in range(1, 8):
        along(step).start()
    total = zout[z]
    for step in range(1, 8):
        along(step).wait_recv()
        total = total + zin[step - 1]
    zall[z] = total
    for step in range(1, 8):
        back(step).start()
    for step in range(1, 8):
        back(step).wait_recv()

    def gather(t, s):
        size = 16 >> t
        here = full.at[s, pl.ds(starts[s][t + 1], size)]
        source = zall.at[pl.ds(2 * s, 2)] if t == 3 else here
        return remote(source, here, a_send.at[t, s], a_recv.at[t, s], links[(s + t) % 4][0])

    for s in range(4):
        gather(3, s).start()
    for s in range(4):
        full[s, pl.ds(starts[s][4], 2)] = zall[pl.ds(2 * s, 2)]
    for t in (2, 1, 0):
        for s in range(4):
            gather(t + 1, s).wait_recv()
            gather(t, s).start()

    def add_gram(rows, first):
        part_high, part_low = split(rows)
        for i in range(5):
            lo = 128 * i
            value = None
            for left in (part_low, part_high):
                for right in (part_low, part_high):
                    term = lax.dot_general(
                        left[:, lo:lo + 128], right[:, lo:], (((0,), (0,)), ((), ())), preferred_element_type=F32
                    )
                    value = term if value is None else value + term
            if first:
                mine[lo:lo + 128, lo:] = value
            else:
                mine[lo:lo + 128, lo:] += value

    add_gram(jnp.concatenate([full[s, pl.ds(starts[s][1], 16)].reshape(128, 640) for s in range(4)], axis=0), True)
    for s in (0, 2):
        rows = []
        for u in (s, s + 1):
            gather(0, u).wait_recv()
            rows.append(full[u, pl.ds(sent[u][0], 16)].reshape(128, 640))
        add_gram(jnp.concatenate(rows, axis=0), False)

    def swap(i):
        lo = 128 * i
        return remote(
            mine.at[pl.ds(lo, 128), pl.ds(lo, 640 - lo)], other.at[pl.ds(lo, 128), pl.ds(lo, 640 - lo)],
            m_send.at[i], m_recv.at[i], peer,
        )

    for i in range(5):
        swap(i).start()
    for i in range(5):
        lo = 128 * i
        swap(i).wait_recv()
        out[lo:lo + 128, lo:] = mine[lo:lo + 128, lo:] + other[lo:lo + 128, lo:]
        if i:
            out[lo:lo + 128, :lo] = jnp.zeros((128, lo), F32)

    for i in range(8):
        chunk(i).wait_send()
    for t in range(4):
        for s in range(4):
            scatter(t, s).wait_send()
            gather(t, s).wait_send()
    for step in range(1, 8):
        along(step).wait_send()
        back(step).wait_send()
    for i in range(5):
        swap(i).wait_send()


def sketch_gram(sketch, wide):
    dma = pltpu.SemaphoreType.DMA
    scratch = [pltpu.VMEM((256, 640), BF16)] * 2
    scratch += [pltpu.VMEM((4, 32, 8, 640), F32)] * 3
    scratch += [pltpu.VMEM((4, 16 >> t, 8, 640), F32) for t in range(4)]
    scratch += [pltpu.VMEM((8, 8, 640), F32), pltpu.VMEM((7, 8, 640), F32), pltpu.VMEM((8, 8, 640), F32)]
    scratch += [pltpu.VMEM((4, 32, 8, 640), F32)]
    scratch += [pltpu.VMEM((640, 640), F32)] * 2
    scratch += [dma((8,))] * 2 + [dma((4, 4))] * 2 + [dma((7,))] * 4 + [dma((4, 4))] * 2 + [dma((5,))] * 2
    return pl.pallas_call(
        gram_kernel,
        out_shape=jax.ShapeDtypeStruct((640, 640), F32),
        in_specs=[vmem()] * 2,
        out_specs=vmem(),
        scratch_shapes=scratch,
        compiler_params=pltpu.CompilerParams(
            collective_id=0, has_side_effects=True, vmem_limit_bytes=48 * 1024 * 1024
        ),
        name="sketch_gram",
    )(sketch, wide)


def sweep(blocks, panels):
    blocks = list(blocks)
    lane = lax.broadcasted_iota(jnp.int32, (8, 128), 1)
    row = lax.broadcasted_iota(jnp.int32, (8, 128), 0)
    for p in range(panels):
        k = 8 * p
        inside = (lane >= k) & (lane < k + 8)
        cols = [[jnp.broadcast_to(b[:, k + s:k + s + 1], (8, 128)) for s in range(8)] for b in blocks]
        e = list(cols[p])
        r = jnp.where(inside, (lane - k == row).astype(F32), blocks[p])
        for s in range(8):
            inv = 1.0 / e[s][s:s + 1, :]
            rs = r[s:s + 1, :] * inv
            r = jnp.where(row == s, rs, r - e[s] * rs)
            for u in range(s + 1, 8):
                es = e[u][s:s + 1, :] * inv
                e[u] = jnp.where(row == s, es, e[u] - e[s] * es)
        rows = [r[s:s + 1, :] for s in range(8)]
        for i in range(len(blocks)):
            if i == p:
                continue
            total = jnp.where(inside, 0.0, blocks[i])
            for s in range(8):
                total = total - cols[i][s] * rows[s]
            blocks[i] = total
        blocks[p] = r
    return blocks


def solve_kernel(count, gram, wide, coef, resid, small, a):
    r = lax.broadcasted_iota(jnp.int32, (128, 128), 0)
    c = lax.broadcasted_iota(jnp.int32, (128, 128), 1)
    a[...] = gram[...]
    for k in range(4):
        lo = 128 * k
        hi = lo + 128
        unused = (c + lo >= count[0]) & (r == c)
        block = a[lo:hi, lo:hi] + jnp.where(unused, 1.0, 0.0)
        inverse = jnp.concatenate(sweep([block[8 * i:8 * i + 8] for i in range(16)], 16), axis=0)
        y = dot(inverse, a[lo:hi, hi:])
        for i in range(k + 1, 5):
            left = 128 * i
            a[left:left + 128, left:] -= dot_rows(a[lo:hi, left:left + 128], y[:, left - hi:])
        if k:
            a[:lo, hi:] -= dot(a[:lo, lo:hi], y)
        a[lo:hi, hi:] = y
    coefs = a[:512, 512:]
    tail = a[512:, 512:]
    both = jnp.concatenate(sweep([tail[8 * i:8 * i + 8] for i in range(8)], 8), axis=0)
    ratio = both[:, P_SIZE:]
    coef[0:512, :] = coefs
    coef[512:576, :] = both
    left = wide[:, 512:] - dot(wide[:, :512], coefs)
    first = left[:, :P_SIZE]
    second = left[:, P_SIZE:] - dot(first, ratio)
    final = jnp.concatenate([first, second], axis=1)
    resid[...] = final
    own = dot_rows(final, final)
    small[...] = jnp.concatenate([own[:P_SIZE, :P_SIZE], own[P_SIZE:, P_SIZE:]], axis=1)


def solve(count, gram, wide):
    return pl.pallas_call(
        solve_kernel,
        out_shape=(
            jax.ShapeDtypeStruct((576, 128), F32),
            jax.ShapeDtypeStruct((256, 128), F32),
            jax.ShapeDtypeStruct((64, 128), F32),
        ),
        in_specs=[pl.BlockSpec(memory_space=pltpu.SMEM), vmem(), vmem()],
        out_specs=(vmem(),) * 3,
        scratch_shapes=[pltpu.VMEM((640, 640), F32)],
        compiler_params=pltpu.CompilerParams(vmem_limit_bytes=32 * 1024 * 1024),
        name="solve",
    )(count, gram, wide)


def sum_kernel(small, out, peer_in, half, x_in, xy, y_in, xyz, z_in, done,
               p_send, p_recv, x_send, x_recv, y_send, y_recv, z_send, z_recv, b_send, b_recv):
    x, z, y, c = (lax.axis_index(name) for name in AXES)
    peer = {"c": 1 - c}
    xs = [{"x": lax.rem(x + step, 4)} for step in range(1, 4)]
    ys = [{"y": lax.rem(y + step, 4)} for step in range(1, 4)]
    zs = [{"z": lax.rem(z + step, 8)} for step in range(1, 8)]
    barrier = pltpu.get_barrier_semaphore()
    for target in [peer] + xs + ys + zs:
        pl.semaphore_signal(barrier, inc=1, device_id=target, device_id_type=MESH)
    pl.semaphore_wait(barrier, 14)

    def remote(source, target, send, recv, device):
        return pltpu.make_async_remote_copy(
            src_ref=source, dst_ref=target, send_sem=send, recv_sem=recv, device_id=device, device_id_type=MESH
        )

    def exchange(source, target, send, recv, devices):
        return [remote(source, target.at[i], send.at[i], recv.at[i], device) for i, device in enumerate(devices)]

    theirs = pl.ds(pl.multiple_of(32 * (1 - c), 32), 32)
    ours = pl.ds(pl.multiple_of(32 * c, 32), 32)
    across = remote(small.at[theirs], peer_in, p_send, p_recv, peer)
    across.start()
    across.wait_recv()
    half[...] = small[ours, :] + peer_in[...]
    on_x = exchange(half, x_in, x_send, x_recv, xs)
    for copy in on_x:
        copy.start()
    for copy in on_x:
        copy.wait_recv()
    xy[...] = half[...] + x_in[0] + x_in[1] + x_in[2]
    on_y = exchange(xy, y_in, y_send, y_recv, ys)
    for copy in on_y:
        copy.start()
    for copy in on_y:
        copy.wait_recv()
    xyz[...] = xy[...] + y_in[0] + y_in[1] + y_in[2]
    on_z = exchange(xyz, z_in, z_send, z_recv, zs)
    for copy in on_z:
        copy.start()
    total = xyz[...]
    for copy in on_z:
        copy.wait_recv()
    for i in range(7):
        total = total + z_in[i]
    done[...] = total
    out[ours, :] = total
    back = remote(done, out.at[ours], b_send, b_recv, peer)
    back.start()
    back.wait_recv()
    for copy in [across, back] + on_x + on_y + on_z:
        copy.wait_send()


def sum_small(small):
    dma = pltpu.SemaphoreType.DMA
    block = (32, 128)
    return pl.pallas_call(
        sum_kernel,
        out_shape=jax.ShapeDtypeStruct((64, 128), F32),
        in_specs=[vmem()],
        out_specs=vmem(),
        scratch_shapes=[
            pltpu.VMEM(block, F32), pltpu.VMEM(block, F32), pltpu.VMEM((3,) + block, F32), pltpu.VMEM(block, F32),
            pltpu.VMEM((3,) + block, F32), pltpu.VMEM(block, F32), pltpu.VMEM((7,) + block, F32), pltpu.VMEM(block, F32),
            dma, dma, dma((3,)), dma((3,)), dma((3,)), dma((3,)), dma((7,)), dma((7,)), dma, dma,
        ],
        compiler_params=pltpu.CompilerParams(collective_id=1, has_side_effects=True),
        name="sum_small",
    )(small)


def finish_kernel(scale, small, coef, resid, basis, factors):
    lane = lax.broadcasted_iota(jnp.int32, (8, 128), 1)
    row = lax.broadcasted_iota(jnp.int32, (8, 128), 0)
    left = lane < P_SIZE
    place = jnp.where(left, lane, lane - P_SIZE)
    blocks = [small[8 * i:8 * i + 8, :] for i in range(8)]
    extra = [(place == row + 8 * i).astype(F32) for i in range(8)]
    roots, inverses = [], []
    for p in range(8):
        k = 8 * p

        def column(block, s):
            first = jnp.broadcast_to(block[:, k + s:k + s + 1], (8, 128))
            second = jnp.broadcast_to(block[:, P_SIZE + k + s:P_SIZE + k + s + 1], (8, 128))
            return jnp.where(left, first, second)

        cols = {i: [column(blocks[i], s) for s in range(8)] for i in range(p, 8)}
        e = list(cols[p])
        r, q = blocks[p], extra[p]
        for s in range(8):
            pivot = e[s][s:s + 1, :]
            inv = 1.0 / pivot
            root = lax.rsqrt(pivot)
            roots.append(jnp.where(place[:1] >= k + s, r[s:s + 1, :] * root, 0.0))
            inverses.append(q[s:s + 1, :] * root)
            rs, qs = r[s:s + 1, :] * inv, q[s:s + 1, :] * inv
            here = row == s
            r = jnp.where(here, rs, r - e[s] * rs)
            q = jnp.where(here, qs, q - e[s] * qs)
            for u in range(s + 1, 8):
                es = e[u][s:s + 1, :] * inv
                e[u] = jnp.where(here, es, e[u] - e[s] * es)
        for i in range(p + 1, 8):
            for s in range(8):
                blocks[i] = blocks[i] - cols[i][s] * r[s:s + 1, :]
                extra[i] = extra[i] - cols[i][s] * q[s:s + 1, :]
    tri = jnp.concatenate(roots, axis=0)
    inverse = jnp.concatenate(inverses, axis=0)
    on_left = lax.broadcasted_iota(jnp.int32, (64, 128), 1) < P_SIZE
    both = jnp.concatenate([jnp.where(on_left, inverse, 0.0), jnp.where(on_left, 0.0, inverse)], axis=0)
    basis[...] = scale * lax.dot_general(
        resid[...], both, (((1,), (1,)), ((), ())), precision=lax.Precision.HIGHEST, preferred_element_type=F32
    )
    tri_one = jnp.where(on_left, tri, 0.0)
    ratio = jnp.where(on_left, 0.0, coef[512:576, :])
    factors[0:512, :] = coef[0:512, :]
    factors[512:576, :] = tri_one + dot(tri_one[:, :P_SIZE], ratio)
    factors[576:640, :] = jnp.where(on_left, 0.0, tri)


def finish(scale, small, coef, resid):
    return pl.pallas_call(
        functools.partial(finish_kernel, scale),
        out_shape=(jax.ShapeDtypeStruct((256, 128), F32), jax.ShapeDtypeStruct((640, 128), F32)),
        in_specs=[vmem()] * 3,
        out_specs=(vmem(),) * 2,
        name="finish",
    )(small, coef, resid)


def shards(sketch, prior_basis, panel_block, panel_index, prior_count):
    width = prior_basis.shape[1]
    column_keep = (jnp.arange(width) < prior_count[0]).astype(F32)
    chosen = lax.dynamic_slice_in_dim(panel_block, panel_index[0] * P_SIZE, 2 * P_SIZE, 1)
    wide = jnp.concatenate([prior_basis * column_keep, chosen], axis=1)
    gram = sketch_gram(sketch, wide)
    coef, resid, small = solve(prior_count, gram, wide)
    scale = math.sqrt(prior_basis.shape[0] * 256)
    return finish(scale, sum_small(small), coef, resid)


def solution(mesh):
    torus = Mesh(mesh.devices.reshape(4, 8, 4, 2), AXES)
    return jax.shard_map(
        shards,
        mesh=torus,
        in_specs=(P(None, AXES), P(AXES, None), P(AXES, None), P(), P()),
        out_specs=(P(AXES, None), P()),
        check_vma=False,
    )
```

```python
import functools
import math

import jax
import jax.numpy as jnp
from jax import lax
from jax.experimental import pallas as pl
from jax.experimental.pallas import tpu as pltpu
from jax.sharding import Mesh
from jax.sharding import PartitionSpec as P

P_SIZE = 64
AXES = ("x", "z", "y", "c")
MESH = pl.DeviceIdType.MESH
F32 = jnp.float32
BF16 = jnp.bfloat16


def vmem():
    return pl.BlockSpec(memory_space=pltpu.VMEM)


def dot(left, right):
    return jnp.dot(left, right, precision=lax.Precision.HIGHEST, preferred_element_type=F32)


def dot_rows(left, right):
    return lax.dot_general(
        left, right, (((0,), (0,)), ((), ())), precision=lax.Precision.HIGHEST, preferred_element_type=F32
    )


def split(value):
    high = value.astype(BF16)
    return high, (value - high.astype(F32)).astype(BF16)


def halves(place):
    first = (place + 1) - 2 * lax.rem(place, 2)
    second = lax.rem(place + 3 + 2 * lax.rem(place, 2), 4)
    return (first, lax.rem((place + 1) // 2, 2)), (second, place // 2)


def square(part_high, part_low, lo):
    value = None
    for left in (part_low, part_high):
        for right in (part_low, part_high):
            term = lax.dot_general(
                left[:, lo:lo + 128], right[:, lo:], (((0,), (0,)), ((), ())), preferred_element_type=F32
            )
            value = term if value is None else value + term
    return value


def choose(panel, index):
    return jnp.where(
        index == 0, panel[:, 0:128], jnp.where(index == 1, panel[:, 64:192], panel[:, 128:256])
    )


ARRIVALS = (0, 1, 7, 2, 6, 3, 5, 4)
BLOCKS = [(i, j) for i in range(5) for j in range(i, 5)]
TILE = (8, 768)
NEAREST_FIRST = (1, 7, 2, 6, 3, 5, 4)


def gram_kernel(count, index, sketch_hbm, prior_hbm, panel_hbm, out, plain, sketch, prior, panel, high, low, dense, away, came, acc,
                r0, r1, r2, r3, zout, zin, zall, full, mine, other, load,
                d_send, d_recv, r_send, r_recv, z_send, z_recv, y_send, y_recv, a_send, a_recv, m_send, m_recv, b_send, b_recv):
    loads = [pltpu.make_async_copy(prior_hbm, prior, load.at[0]), pltpu.make_async_copy(panel_hbm, panel, load.at[1])]
    for i in range(8):
        rows = pl.ds(256 * i, 256)
        loads.append(pltpu.make_async_copy(sketch_hbm.at[rows], sketch.at[rows], load.at[2 + i]))
    for copy in loads:
        copy.start()

    x, z, y, c = (lax.axis_index(name) for name in AXES)
    (xa, xa_bit), (xb, xb_bit) = halves(x)
    (ya, ya_bit), (yb, yb_bit) = halves(y)
    bits = (xa_bit, ya_bit, xb_bit, yb_bit)
    links = ({"x": xa}, {"y": ya}, {"x": xb}, {"y": yb})
    ring = [{"z": lax.rem(z + step, 8)} for step in range(1, 8)]
    peer = {"c": 1 - c}

    barrier = pltpu.get_barrier_semaphore()
    for target in [peer] + list(links) + ring:
        pl.semaphore_signal(barrier, inc=1, device_id=target, device_id_type=MESH)

    def remote(source, target, send, recv, device):
        return pltpu.make_async_remote_copy(
            src_ref=source, dst_ref=target, send_sem=send, recv_sem=recv, device_id=device, device_id_type=MESH
        )

    def kept(s, t, bits=bits):
        return sum([bits[(s + u) % 4] * (8 >> u) for u in range(t)], jnp.int32(0))

    def gone(s, t, bits=bits):
        return kept(s, t, bits) + (1 - bits[(s + t) % 4]) * (8 >> t)

    turned_bits, turned_links = [], []
    for turn in range(4):
        link = lax.rem(z + turn, 4)
        upper, odd = link // 2, lax.rem(link, 2)

        def pick(values):
            return (1 - upper) * ((1 - odd) * values[0] + odd * values[1]) + upper * (
                (1 - odd) * values[2] + odd * values[3]
            )

        turned_bits.append(pick(bits))
        turned_links.append({"x": pick((xa, x, xb, x)), "y": pick((y, ya, y, yb))})

    for copy in loads[:2]:
        copy.wait()
    keep = lax.broadcasted_iota(jnp.int32, (256, 512), 1) < count[0]
    high[:, :512], low[:, :512] = split(jnp.where(keep, prior[...], 0.0))
    high[:, 512:], low[:, 512:] = split(choose(panel, index[0]))
    for i in range(5):
        lo = 128 * i
        value = square(high, low, lo)
        for j in range(i, 5):
            at = 128 * (j - i)
            dense[BLOCKS.index((i, j))] = value[:, at:at + 128].reshape(16, 8, 128)
    dense[15] = jnp.zeros((16, 8, 128), F32)
    for copy in loads[2:]:
        copy.wait()

    def product(core, tiles, target):
        rows = [sketch[pl.ds(pl.multiple_of(core * 1024 + s * 128 + tiles[s] * 8, 64), 64), :] for s in range(8)]
        part_high, part_low = split(jnp.concatenate(rows, axis=0))
        value = jnp.dot(part_high, low[...], preferred_element_type=F32)
        value = value + jnp.dot(part_low, high[...], preferred_element_type=F32)
        value = value + jnp.dot(part_high, high[...], preferred_element_type=F32)
        for s in range(8):
            target[s, pl.ds(tiles[s], 8), :, :640] = value[64 * s:64 * s + 64].reshape(8, 8, 640)
            target[s, pl.ds(tiles[s], 8), :, 640:] = dense[core * 8 + s, pl.ds(tiles[s], 8)]

    parts = ([gone(s, 0) for s in range(8)], [kept(s, 1) for s in range(8)])

    def chunk(part, s):
        tile = parts[part][s]
        return remote(
            away.at[s, pl.ds(tile, 8)], came.at[s, pl.ds(tile, 8)], d_send.at[part, s], d_recv.at[part, s], peer
        )

    for part in range(2):
        product(1 - c, parts[part], away)
    product(c, parts[0], acc)
    pl.semaphore_wait(barrier, 12)
    for part in range(2):
        for s in range(8):
            chunk(part, s).start()
    product(c, parts[1], acc)

    landing = (r0, r1, r2, r3)

    def scatter(t, s):
        size = 8 >> t
        return remote(
            acc.at[s, pl.ds(gone(s, t), size)], landing[t].at[s], r_send.at[t, s], r_recv.at[t, s],
            links[(s + t) % 4],
        )

    def along(s):
        return remote(zout.at[s], zin.at[z], z_send.at[s], z_recv.at[z], {"z": jnp.int32(s)})

    for part in range(2):
        for s in range(8):
            chunk(part, s).wait_recv()
            acc[s, pl.ds(parts[part][s], 8)] += came[s, pl.ds(parts[part][s], 8)]
            if part == 0:
                scatter(0, s).start()
    for t in range(4):
        size = 8 >> t
        for s in range(8):
            scatter(t, s).wait_recv()
            at = kept(s, t + 1)
            if t < 3:
                acc[s, pl.ds(at, size)] += landing[t][s]
                scatter(t + 1, s).start()
            else:
                zout[pl.ds(s, 1)] = acc[s, pl.ds(at, 1)] + r3[s]

                @pl.when(z != s)
                def _():
                    along(s).start()

    total = zout[z]
    for step in range(1, 8):
        source = lax.rem(z + step, 8)
        remote(zout.at[0], zin.at[source], z_send.at[0], z_recv.at[source], ring[0]).wait_recv()
        total = total + zin[source]
    zall[0] = total

    def back(step):
        return remote(zall.at[0], zall.at[8 - step], y_send.at[step - 1], y_recv.at[step - 1], ring[step - 1])

    for step in NEAREST_FIRST:
        back(step).start()

    def gather(t, s):
        here = full.at[s, pl.ds(kept(s, t + 1, turned_bits), 8 >> t)]
        source = zall.at[pl.ds(s, 1)] if t == 3 else here
        return remote(source, here, a_send.at[t, s], a_recv.at[t, s], turned_links[(s + t) % 4])

    for s in ARRIVALS:
        if s:
            back(8 - s).wait_recv()
        gather(3, s).start()
        full[s, pl.ds(kept(s, 4, turned_bits), 1)] = zall[pl.ds(s, 1)]
    for t in (3, 2, 1):
        for s in ARRIVALS:
            gather(t, s).wait_recv()
            gather(t - 1, s).start()

    def swap(i):
        lo = 128 * i
        place = (pl.ds(lo, 128), pl.ds(lo, 640 - lo))
        return remote(mine.at[place], other.at[place], m_send.at[i], m_recv.at[i], peer)

    ours = pl.ds(8 * c, 8)
    trade = remote(plain.at[ours], plain.at[ours], b_send, b_recv, peer)

    def add_gram(rows, first, last):
        part_high, part_low = split(rows)
        for i in range(5):
            lo = 128 * i
            value = square(part_high, part_low, lo)
            if first:
                mine[lo:lo + 128, lo:] = value
            else:
                mine[lo:lo + 128, lo:] += value
            if last:
                swap(i).start()

    def part_of(s, at):
        return full[s, pl.ds(at, 8), :, :640].reshape(64, 640)

    add_gram(jnp.concatenate([part_of(s, kept(s, 1, turned_bits)) for s in range(8)], axis=0), True, False)
    for last, some in ((False, ARRIVALS[:4]), (True, ARRIVALS[4:])):
        rows = []
        for s in some:
            gather(0, s).wait_recv()
            rows.append(part_of(s, gone(s, 0, turned_bits)))
            plain[8 * c + lax.rem(z + s, 8)] = full[s, :, :, 640:]
        if last:
            trade.start()
        add_gram(jnp.concatenate(rows, axis=0), False, last)
    for i in range(5):
        lo = 128 * i
        swap(i).wait_recv()
        out[lo:lo + 128, lo:] = mine[lo:lo + 128, lo:] + other[lo:lo + 128, lo:]
    trade.wait_recv()

    for s in range(8):
        for part in range(2):
            chunk(part, s).wait_send()
        for t in range(4):
            scatter(t, s).wait_send()
            gather(t, s).wait_send()

        @pl.when(z != s)
        def _():
            along(s).wait_send()

    for step in range(1, 8):
        back(step).wait_send()
    for i in range(5):
        swap(i).wait_send()
    trade.wait_send()


def sketch_gram(count, index, sketch, prior, panel):
    dma = pltpu.SemaphoreType.DMA
    stream = (8, 16) + TILE
    scratch = [pltpu.VMEM((2048, 256), F32), pltpu.VMEM((256, 512), F32), pltpu.VMEM((256, 256), F32)]
    scratch += [pltpu.VMEM((256, 640), BF16)] * 2 + [pltpu.VMEM((16, 16, 8, 128), F32)]
    scratch += [pltpu.VMEM(stream, F32)] * 3
    scratch += [pltpu.VMEM((8, 8 >> t) + TILE, F32) for t in range(4)]
    scratch += [pltpu.VMEM((8,) + TILE, F32)] * 3
    scratch += [pltpu.VMEM(stream, F32)]
    scratch += [pltpu.VMEM((640, 640), F32)] * 2
    scratch += [dma((10,))] + [dma((2, 8))] * 2 + [dma((4, 8))] * 2
    scratch += [dma((8,))] * 2 + [dma((7,))] * 2 + [dma((4, 8))] * 2 + [dma((5,))] * 2 + [dma] * 2
    smem = pl.BlockSpec(memory_space=pltpu.SMEM)
    hbm = pl.BlockSpec(memory_space=pl.ANY)
    return pl.pallas_call(
        gram_kernel,
        out_shape=(jax.ShapeDtypeStruct((640, 640), F32), jax.ShapeDtypeStruct((16, 16, 8, 128), F32)),
        in_specs=[smem, smem, hbm, hbm, hbm],
        out_specs=(vmem(),) * 2,
        scratch_shapes=scratch,
        compiler_params=pltpu.CompilerParams(
            collective_id=0, has_side_effects=True, vmem_limit_bytes=56 * 1024 * 1024
        ),
        name="sketch_gram",
    )(count, index, sketch, prior, panel)


def sweep(blocks, panels):
    blocks = list(blocks)
    lane = lax.broadcasted_iota(jnp.int32, (8, 128), 1)
    row = lax.broadcasted_iota(jnp.int32, (8, 128), 0)
    for p in range(panels):
        k = 8 * p
        inside = (lane >= k) & (lane < k + 8)
        cols = [[jnp.broadcast_to(b[:, k + s:k + s + 1], (8, 128)) for s in range(8)] for b in blocks]
        e = list(cols[p])
        r = jnp.where(inside, (lane - k == row).astype(F32), blocks[p])
        for s in range(8):
            inv = 1.0 / e[s][s:s + 1, :]
            rs = r[s:s + 1, :] * inv
            r = jnp.where(row == s, rs, r - e[s] * rs)
            for u in range(s + 1, 8):
                es = e[u][s:s + 1, :] * inv
                e[u] = jnp.where(row == s, es, e[u] - e[s] * es)
        rows = [r[s:s + 1, :] for s in range(8)]
        for i in range(len(blocks)):
            if i == p:
                continue
            total = jnp.where(inside, 0.0, blocks[i])
            for s in range(8):
                total = total - cols[i][s] * rows[s]
            blocks[i] = total
        blocks[p] = r
    return blocks


def factor(small):
    lane = lax.broadcasted_iota(jnp.int32, (8, 128), 1)
    row = lax.broadcasted_iota(jnp.int32, (8, 128), 0)
    left = lane < P_SIZE
    place = jnp.where(left, lane, lane - P_SIZE)
    blocks = [small[8 * i:8 * i + 8, :] for i in range(8)]
    extra = [(place == row + 8 * i).astype(F32) for i in range(8)]
    roots, inverses = [], []
    for p in range(8):
        k = 8 * p

        def column(block, s):
            first = jnp.broadcast_to(block[:, k + s:k + s + 1], (8, 128))
            second = jnp.broadcast_to(block[:, P_SIZE + k + s:P_SIZE + k + s + 1], (8, 128))
            return jnp.where(left, first, second)

        cols = {i: [column(blocks[i], s) for s in range(8)] for i in range(p, 8)}
        e = list(cols[p])
        r, q = blocks[p], extra[p]
        for s in range(8):
            pivot = e[s][s:s + 1, :]
            inv = 1.0 / pivot
            root = lax.rsqrt(pivot)
            roots.append(jnp.where(place[:1] >= k + s, r[s:s + 1, :] * root, 0.0))
            inverses.append(q[s:s + 1, :] * root)
            rs, qs = r[s:s + 1, :] * inv, q[s:s + 1, :] * inv
            here = row == s
            r = jnp.where(here, rs, r - e[s] * rs)
            q = jnp.where(here, qs, q - e[s] * qs)
            for u in range(s + 1, 8):
                es = e[u][s:s + 1, :] * inv
                e[u] = jnp.where(here, es, e[u] - e[s] * es)
        for i in range(p + 1, 8):
            for s in range(8):
                blocks[i] = blocks[i] - cols[i][s] * r[s:s + 1, :]
                extra[i] = extra[i] - cols[i][s] * q[s:s + 1, :]
    return jnp.concatenate(roots, axis=0), jnp.concatenate(inverses, axis=0)


def project_kernel(scale, count, index, gram, plain, prior, panel, basis, factors, a, b):
    r = lax.broadcasted_iota(jnp.int32, (128, 128), 0)
    c = lax.broadcasted_iota(jnp.int32, (128, 128), 1)
    on_left = lax.broadcasted_iota(jnp.int32, (64, 128), 1) < P_SIZE
    for at, (i, j) in enumerate(BLOCKS):
        block = plain[at].reshape(128, 128)
        b[128 * i:128 * i + 128, 128 * j:128 * j + 128] = block
        if i != j:
            b[128 * j:128 * j + 128, 128 * i:128 * i + 128] = block.T
    for i in range(5):
        a[128 * i:128 * i + 128, 128 * i:] = gram[128 * i:128 * i + 128, 128 * i:]
    for k in range(4):
        lo = 128 * k
        hi = lo + 128
        unused = (c + lo >= count[0]) & (r == c)
        block = a[lo:hi, lo:hi] + jnp.where(unused, 1.0, 0.0)
        inverse = jnp.concatenate(sweep([block[8 * i:8 * i + 8] for i in range(16)], 16), axis=0)
        y = dot(inverse, a[lo:hi, hi:])
        for i in range(k + 1, 5):
            left = 128 * i
            a[left:left + 128, left:] -= dot_rows(a[lo:hi, left:left + 128], y[:, left - hi:])
        if k:
            a[:lo, hi:] -= dot(a[:lo, lo:hi], y)
        a[lo:hi, hi:] = y
    coefs = a[:512, 512:]
    tail = a[512:, 512:]
    both = jnp.concatenate(sweep([tail[8 * i:8 * i + 8] for i in range(8)], 8), axis=0)
    ratio = jnp.where(on_left, 0.0, both)
    ends = (r == c).astype(F32) - jnp.concatenate([ratio, jnp.zeros((64, 128), F32)], axis=0)
    weights = jnp.concatenate([dot(coefs[:, :P_SIZE], ratio) - coefs, ends], axis=0)
    own = dot_rows(weights, dot(b[...], weights))
    small = jnp.concatenate([own[:P_SIZE, :P_SIZE], own[P_SIZE:, P_SIZE:]], axis=1)
    keep = lax.broadcasted_iota(jnp.int32, (256, 512), 1) < count[0]
    resid = choose(panel, index[0]) - dot(jnp.where(keep, prior[...], 0.0), coefs)
    resid = resid - dot(resid[:, :P_SIZE], ratio)
    tri, inverse = factor(small)
    both = jnp.concatenate([jnp.where(on_left, inverse, 0.0), jnp.where(on_left, 0.0, inverse)], axis=0)
    basis[...] = scale * lax.dot_general(
        resid, both, (((1,), (1,)), ((), ())), precision=lax.Precision.HIGHEST, preferred_element_type=F32
    )
    tri_one = jnp.where(on_left, tri, 0.0)
    factors[0:512, :] = coefs
    factors[512:576, :] = tri_one + dot(tri_one[:, :P_SIZE], ratio)
    factors[576:640, :] = jnp.where(on_left, 0.0, tri)


def project(scale, count, index, gram, plain, prior, panel):
    return pl.pallas_call(
        functools.partial(project_kernel, scale),
        out_shape=(jax.ShapeDtypeStruct((256, 128), F32), jax.ShapeDtypeStruct((640, 128), F32)),
        in_specs=[pl.BlockSpec(memory_space=pltpu.SMEM)] * 2 + [vmem()] * 4,
        out_specs=(vmem(),) * 2,
        scratch_shapes=[pltpu.VMEM((640, 640), F32)] * 2,
        compiler_params=pltpu.CompilerParams(vmem_limit_bytes=32 * 1024 * 1024),
        name="project",
    )(count, index, gram, plain, prior, panel)


def shards(sketch, prior_basis, panel_block, panel_index, prior_count):
    gram, plain = sketch_gram(prior_count, panel_index, sketch, prior_basis, panel_block)
    scale = math.sqrt(prior_basis.shape[0] * 256)
    return project(scale, prior_count, panel_index, gram, plain, prior_basis, panel_block)


def solution(mesh):
    torus = Mesh(mesh.devices.reshape(4, 8, 4, 2), AXES)
    return jax.shard_map(
        shards,
        mesh=torus,
        in_specs=(P(None, AXES), P(AXES, None), P(AXES, None), P(), P()),
        out_specs=(P(AXES, None), P()),
        check_vma=False,
    )
```

```python
import functools
import math

import jax
import jax.numpy as jnp
from jax import lax
from jax.experimental import pallas as pl
from jax.experimental.pallas import tpu as pltpu
from jax.sharding import Mesh
from jax.sharding import PartitionSpec as P

P_SIZE = 64
AXES = ("x", "z", "y", "c")
MESH = pl.DeviceIdType.MESH
F32 = jnp.float32
BF16 = jnp.bfloat16


def vmem():
    return pl.BlockSpec(memory_space=pltpu.VMEM)


def dot(left, right):
    return jnp.dot(left, right, precision=lax.Precision.HIGHEST, preferred_element_type=F32)


def dot_rows(left, right):
    return lax.dot_general(
        left, right, (((0,), (0,)), ((), ())), precision=lax.Precision.HIGHEST, preferred_element_type=F32
    )


def split(value):
    high = value.astype(BF16)
    return high, (value - high.astype(F32)).astype(BF16)


def halves(place):
    first = (place + 1) - 2 * lax.rem(place, 2)
    second = lax.rem(place + 3 + 2 * lax.rem(place, 2), 4)
    return (first, lax.rem((place + 1) // 2, 2)), (second, place // 2)


def square(part_high, part_low, lo):
    value = None
    for left in (part_low, part_high):
        for right in (part_low, part_high):
            term = lax.dot_general(
                left[:, lo:lo + 128], right[:, lo:], (((0,), (0,)), ((), ())), preferred_element_type=F32
            )
            value = term if value is None else value + term
    return value


def choose(panel, index):
    return jnp.where(
        index == 0, panel[:, 0:128], jnp.where(index == 1, panel[:, 64:192], panel[:, 128:256])
    )


ARRIVALS = (0, 1, 7, 2, 6, 3, 5, 4)
BLOCKS = [(i, j) for i in range(5) for j in range(i, 5)]
TILE = (8, 768)
NEAREST_FIRST = (1, 7, 2, 6, 3, 5, 4)


def gram_kernel(count, index, sketch_hbm, prior_hbm, panel_hbm, out, plain, sketch, prior, panel, high, low, dense, away, came, acc,
                r0, r1, r2, zout, zin, zall, full, mine, other, load,
                d_send, d_recv, r_send, r_recv, z_send, z_recv, y_send, y_recv, a_send, a_recv, m_send, m_recv, b_send, b_recv):
    loads = [pltpu.make_async_copy(prior_hbm, prior, load.at[0]), pltpu.make_async_copy(panel_hbm, panel, load.at[1])]
    for i in range(8):
        rows = pl.ds(256 * i, 256)
        loads.append(pltpu.make_async_copy(sketch_hbm.at[rows], sketch.at[rows], load.at[2 + i]))
    for copy in loads:
        copy.start()

    x, z, y, c = (lax.axis_index(name) for name in AXES)
    (xa, xa_bit), (xb, xb_bit) = halves(x)
    (ya, ya_bit), (yb, yb_bit) = halves(y)
    bits = (xa_bit, ya_bit, xb_bit, yb_bit)
    links = ({"x": xa}, {"y": ya}, {"x": xb}, {"y": yb})
    ring = [{"z": lax.rem(z + step, 8)} for step in range(1, 8)]
    peer = {"c": 1 - c}

    barrier = pltpu.get_barrier_semaphore()
    corners = [{**links[i], **links[(i + 1) % 4]} for i in range(4)]
    for target in [peer] + list(links) + corners + ring:
        pl.semaphore_signal(barrier, inc=1, device_id=target, device_id_type=MESH)

    def remote(source, target, send, recv, device):
        return pltpu.make_async_remote_copy(
            src_ref=source, dst_ref=target, send_sem=send, recv_sem=recv, device_id=device, device_id_type=MESH
        )

    def kept(s, t, bits=bits):
        return sum([bits[(s + u) % 4] * (8 >> u) for u in range(t)], jnp.int32(0))

    def gone(s, t, bits=bits):
        return kept(s, t, bits) + (1 - bits[(s + t) % 4]) * (8 >> t)

    turned_bits, turned_links = [], []
    for turn in range(4):
        link = lax.rem(z + turn, 4)
        upper, odd = link // 2, lax.rem(link, 2)

        def pick(values):
            return (1 - upper) * ((1 - odd) * values[0] + odd * values[1]) + upper * (
                (1 - odd) * values[2] + odd * values[3]
            )

        turned_bits.append(pick(bits))
        turned_links.append({"x": pick((xa, x, xb, x)), "y": pick((y, ya, y, yb))})

    for copy in loads[:2]:
        copy.wait()
    keep = lax.broadcasted_iota(jnp.int32, (256, 512), 1) < count[0]
    high[:, :512], low[:, :512] = split(jnp.where(keep, prior[...], 0.0))
    high[:, 512:], low[:, 512:] = split(choose(panel, index[0]))
    for i in range(5):
        lo = 128 * i
        value = square(high, low, lo)
        for j in range(i, 5):
            at = 128 * (j - i)
            dense[BLOCKS.index((i, j))] = value[:, at:at + 128].reshape(16, 8, 128)
    dense[15] = jnp.zeros((16, 8, 128), F32)
    for copy in loads[2:]:
        copy.wait()

    def product(core, tiles, target):
        rows = [sketch[pl.ds(pl.multiple_of(core * 1024 + s * 128 + tiles[s] * 8, 64), 64), :] for s in range(8)]
        part_high, part_low = split(jnp.concatenate(rows, axis=0))
        value = jnp.dot(part_high, low[...], preferred_element_type=F32)
        value = value + jnp.dot(part_low, high[...], preferred_element_type=F32)
        value = value + jnp.dot(part_high, high[...], preferred_element_type=F32)
        for s in range(8):
            target[s, pl.ds(tiles[s], 8), :, :640] = value[64 * s:64 * s + 64].reshape(8, 8, 640)
            target[s, pl.ds(tiles[s], 8), :, 640:] = dense[core * 8 + s, pl.ds(tiles[s], 8)]

    parts = ([gone(s, 0) for s in range(8)], [kept(s, 1) for s in range(8)])

    def chunk(part, s):
        tile = parts[part][s]
        return remote(
            away.at[s, pl.ds(tile, 8)], came.at[s, pl.ds(tile, 8)], d_send.at[part, s], d_recv.at[part, s], peer
        )

    for part in range(2):
        product(1 - c, parts[part], away)
    product(c, parts[0], acc)
    pl.semaphore_wait(barrier, 16)
    for part in range(2):
        for s in range(8):
            chunk(part, s).start()
    product(c, parts[1], acc)

    landing = (r0, r1)

    def scatter(t, s):
        size = 8 >> t
        return remote(
            acc.at[s, pl.ds(gone(s, t), size)], landing[t].at[s], r_send.at[t, s], r_recv.at[t, s],
            links[(s + t) % 4],
        )

    def corner(s, slot):
        over, up = bits[(s + 2) % 4], bits[(s + 3) % 4]
        over = over if slot == 1 else 1 - over
        up = up if slot == 0 else 1 - up
        device = (links[(s + 2) % 4], links[(s + 3) % 4], corners[(s + 2) % 4])[slot]
        return remote(
            acc.at[s, pl.ds(kept(s, 2) + 2 * over + up, 1)], r2.at[s, pl.ds(slot, 1)],
            r_send.at[2 + slot, s], r_recv.at[2 + slot, s], device,
        )

    def along(s):
        return remote(zout.at[s], zin.at[z], z_send.at[s], z_recv.at[z], {"z": jnp.int32(s)})

    for part in range(2):
        for s in range(8):
            chunk(part, s).wait_recv()
            acc[s, pl.ds(parts[part][s], 8)] += came[s, pl.ds(parts[part][s], 8)]
            if part == 0:
                scatter(0, s).start()
    for t in range(2):
        size = 8 >> t
        for s in range(8):
            scatter(t, s).wait_recv()
            acc[s, pl.ds(kept(s, t + 1), size)] += landing[t][s]
            if t == 0:
                scatter(1, s).start()
            else:
                for slot in (2, 0, 1):
                    corner(s, slot).start()
    for s in range(8):
        for slot in range(3):
            corner(s, slot).wait_recv()
        zout[s] = acc[s, kept(s, 4)] + (r2[s, 0] + r2[s, 1] + r2[s, 2])

        @pl.when(z != s)
        def _():
            along(s).start()

    total = zout[z]
    for step in range(1, 8):
        source = lax.rem(z + step, 8)
        remote(zout.at[0], zin.at[source], z_send.at[0], z_recv.at[source], ring[0]).wait_recv()
        total = total + zin[source]
    zall[0] = total

    def back(step):
        return remote(zall.at[0], zall.at[8 - step], y_send.at[step - 1], y_recv.at[step - 1], ring[step - 1])

    for step in NEAREST_FIRST:
        back(step).start()

    def gather(t, s):
        here = full.at[s, pl.ds(kept(s, t + 1, turned_bits), 8 >> t)]
        return remote(here, here, a_send.at[t, s], a_recv.at[t, s], turned_links[(s + t) % 4])

    def gather_corner(s, slot):
        one, two = turned_links[(s + 2) % 4], turned_links[(s + 3) % 4]
        device = (one, two, {"x": one["x"] + two["x"] - x, "y": one["y"] + two["y"] - y})[slot]
        here = full.at[s, pl.ds(kept(s, 4, turned_bits), 1)]
        return remote(zall.at[pl.ds(s, 1)], here, a_send.at[2 + slot, s], a_recv.at[2 + slot, s], device)

    for s in ARRIVALS:
        if s:
            back(8 - s).wait_recv()
        for slot in (2, 0, 1):
            gather_corner(s, slot).start()
        full[s, pl.ds(kept(s, 4, turned_bits), 1)] = zall[pl.ds(s, 1)]
    for s in ARRIVALS:
        for slot in range(3):
            gather_corner(s, slot).wait_recv()
        gather(1, s).start()
    for s in ARRIVALS:
        gather(1, s).wait_recv()
        gather(0, s).start()

    def swap(i):
        lo = 128 * i
        place = (pl.ds(lo, 128), pl.ds(lo, 640 - lo))
        return remote(mine.at[place], other.at[place], m_send.at[i], m_recv.at[i], peer)

    ours = pl.ds(8 * c, 8)
    trade = remote(plain.at[ours], plain.at[ours], b_send, b_recv, peer)

    def add_gram(rows, first, last):
        part_high, part_low = split(rows)
        for i in range(5):
            lo = 128 * i
            value = square(part_high, part_low, lo)
            if first:
                mine[lo:lo + 128, lo:] = value
            else:
                mine[lo:lo + 128, lo:] += value
            if last:
                swap(i).start()

    def part_of(s, at):
        return full[s, pl.ds(at, 8), :, :640].reshape(64, 640)

    add_gram(jnp.concatenate([part_of(s, kept(s, 1, turned_bits)) for s in range(8)], axis=0), True, False)
    for last, some in ((False, ARRIVALS[:4]), (True, ARRIVALS[4:])):
        rows = []
        for s in some:
            gather(0, s).wait_recv()
            rows.append(part_of(s, gone(s, 0, turned_bits)))
            plain[8 * c + lax.rem(z + s, 8)] = full[s, :, :, 640:]
        if last:
            trade.start()
        add_gram(jnp.concatenate(rows, axis=0), False, last)
    for i in range(5):
        lo = 128 * i
        swap(i).wait_recv()
        out[lo:lo + 128, lo:] = mine[lo:lo + 128, lo:] + other[lo:lo + 128, lo:]
    trade.wait_recv()

    for s in range(8):
        for part in range(2):
            chunk(part, s).wait_send()
        for t in range(2):
            scatter(t, s).wait_send()
            gather(t, s).wait_send()
        for slot in range(3):
            corner(s, slot).wait_send()
            gather_corner(s, slot).wait_send()

        @pl.when(z != s)
        def _():
            along(s).wait_send()

    for step in range(1, 8):
        back(step).wait_send()
    for i in range(5):
        swap(i).wait_send()
    trade.wait_send()


def sketch_gram(count, index, sketch, prior, panel):
    dma = pltpu.SemaphoreType.DMA
    stream = (8, 16) + TILE
    scratch = [pltpu.VMEM((2048, 256), F32), pltpu.VMEM((256, 512), F32), pltpu.VMEM((256, 256), F32)]
    scratch += [pltpu.VMEM((256, 640), BF16)] * 2 + [pltpu.VMEM((16, 16, 8, 128), F32)]
    scratch += [pltpu.VMEM(stream, F32)] * 3
    scratch += [pltpu.VMEM((8, size) + TILE, F32) for size in (8, 4, 3)]
    scratch += [pltpu.VMEM((8,) + TILE, F32)] * 3
    scratch += [pltpu.VMEM(stream, F32)]
    scratch += [pltpu.VMEM((640, 640), F32)] * 2
    scratch += [dma((10,))] + [dma((2, 8))] * 2 + [dma((5, 8))] * 2
    scratch += [dma((8,))] * 2 + [dma((7,))] * 2 + [dma((5, 8))] * 2 + [dma((5,))] * 2 + [dma] * 2
    smem = pl.BlockSpec(memory_space=pltpu.SMEM)
    hbm = pl.BlockSpec(memory_space=pltpu.MemorySpace.HBM)
    return pl.pallas_call(
        gram_kernel,
        out_shape=(jax.ShapeDtypeStruct((640, 640), F32), jax.ShapeDtypeStruct((16, 16, 8, 128), F32)),
        in_specs=[smem, smem, hbm, hbm, hbm],
        out_specs=(vmem(),) * 2,
        scratch_shapes=scratch,
        compiler_params=pltpu.CompilerParams(
            collective_id=0, has_side_effects=True, vmem_limit_bytes=50 * 1024 * 1024
        ),
        name="sketch_gram",
    )(count, index, sketch, prior, panel)


def sweep(blocks, first):
    panels = len(blocks)
    blocks = list(blocks)
    lane = lax.broadcasted_iota(jnp.int32, (8, 128), 1)
    row = lax.broadcasted_iota(jnp.int32, (8, 128), 0)

    def columns(block, k):
        return [jnp.broadcast_to(block[:, k + s:k + s + 1], (8, 128)) for s in range(8)]

    e = columns(blocks[0], first)
    for p in range(panels):
        k = first + 8 * p
        inside = (lane >= k) & (lane < k + 8)
        cols = [columns(b, k) if i != p else None for i, b in enumerate(blocks)]
        r = jnp.where(inside, (lane - k == row).astype(F32), blocks[p])
        more = p + 1 < panels
        after = columns(blocks[p], k + 8) if more else []
        following = columns(blocks[p + 1], k + 8) if more else []
        for s in range(8):
            here = row == s
            inv = 1.0 / e[s][s:s + 1, :]

            def step(v):
                own = v[s:s + 1, :] * inv
                return jnp.where(here, own, v - e[s] * own)

            for u in range(s + 1, 8):
                e[u] = step(e[u])
            after = [step(v) for v in after]
            r = step(r)
        if more:
            e = []
            for u in range(8):
                terms = [cols[p + 1][s] * after[u][s:s + 1, :] for s in range(8)]
                while len(terms) > 1:
                    terms = [x + y for x, y in zip(terms[::2], terms[1::2])]
                e.append(following[u] - terms[0])
        for i in range(len(blocks)):
            if i == p:
                continue
            total = jnp.where(inside, 0.0, blocks[i])
            for s in range(8):
                total = total - cols[i][s] * r[s:s + 1, :]
            blocks[i] = total
        blocks[p] = r
    return blocks


def eliminated(rows, first):
    return jnp.concatenate(sweep([rows[8 * i:8 * i + 8] for i in range(8)], first), axis=0)


def inverse_of(block):
    on_left = lax.broadcasted_iota(jnp.int32, (64, 128), 1) < P_SIZE
    top = eliminated(block[:64], 0)
    bottom = jnp.where(on_left, 0.0, block[64:]) - dot(block[64:, :64], top)
    bottom = eliminated(bottom, 64)
    top = jnp.where(on_left, top, 0.0) - dot(top[:, 64:], bottom)
    return jnp.concatenate([top, bottom], axis=0)


def factor(small):
    lane = lax.broadcasted_iota(jnp.int32, (8, 128), 1)
    row = lax.broadcasted_iota(jnp.int32, (8, 128), 0)
    left = lane < P_SIZE
    place = jnp.where(left, lane, lane - P_SIZE)
    blocks = [small[8 * i:8 * i + 8, :] for i in range(8)]
    extra = [(place == row + 8 * i).astype(F32) for i in range(8)]
    roots, inverses = [], []
    for p in range(8):
        k = 8 * p

        def column(block, s):
            first = jnp.broadcast_to(block[:, k + s:k + s + 1], (8, 128))
            second = jnp.broadcast_to(block[:, P_SIZE + k + s:P_SIZE + k + s + 1], (8, 128))
            return jnp.where(left, first, second)

        cols = {i: [column(blocks[i], s) for s in range(8)] for i in range(p, 8)}
        e = list(cols[p])
        r, q = blocks[p], extra[p]
        for s in range(8):
            pivot = e[s][s:s + 1, :]
            inv = 1.0 / pivot
            root = lax.rsqrt(pivot)
            roots.append(jnp.where(place[:1] >= k + s, r[s:s + 1, :] * root, 0.0))
            inverses.append(q[s:s + 1, :] * root)
            rs, qs = r[s:s + 1, :] * inv, q[s:s + 1, :] * inv
            here = row == s
            r = jnp.where(here, rs, r - e[s] * rs)
            q = jnp.where(here, qs, q - e[s] * qs)
            for u in range(s + 1, 8):
                es = e[u][s:s + 1, :] * inv
                e[u] = jnp.where(here, es, e[u] - e[s] * es)
        for i in range(p + 1, 8):
            for s in range(8):
                blocks[i] = blocks[i] - cols[i][s] * r[s:s + 1, :]
                extra[i] = extra[i] - cols[i][s] * q[s:s + 1, :]
    return jnp.concatenate(roots, axis=0), jnp.concatenate(inverses, axis=0)


def project_kernel(scale, count, index, gram, plain, prior, panel, basis, factors, a, b):
    r = lax.broadcasted_iota(jnp.int32, (128, 128), 0)
    c = lax.broadcasted_iota(jnp.int32, (128, 128), 1)
    on_left = lax.broadcasted_iota(jnp.int32, (64, 128), 1) < P_SIZE
    for at, (i, j) in enumerate(BLOCKS):
        block = plain[at].reshape(128, 128)
        b[128 * i:128 * i + 128, 128 * j:128 * j + 128] = block
        if i != j:
            b[128 * j:128 * j + 128, 128 * i:128 * i + 128] = block.T
    for i in range(5):
        a[128 * i:128 * i + 128, 128 * i:] = gram[128 * i:128 * i + 128, 128 * i:]
    for k in range(4):
        lo = 128 * k
        hi = lo + 128
        unused = (c + lo >= count[0]) & (r == c)
        block = a[lo:hi, lo:hi] + jnp.where(unused, 1.0, 0.0)
        y = dot(inverse_of(block), a[lo:hi, hi:])
        for i in range(k + 1, 5):
            left = 128 * i
            a[left:left + 128, left:] -= dot_rows(a[lo:hi, left:left + 128], y[:, left - hi:])
        if k:
            a[:lo, hi:] -= dot(a[:lo, lo:hi], y)
        a[lo:hi, hi:] = y
    coefs = a[:512, 512:]
    tail = a[512:, 512:]
    both = eliminated(tail[:64], 0)
    ratio = jnp.where(on_left, 0.0, both)
    ends = (r == c).astype(F32) - jnp.concatenate([ratio, jnp.zeros((64, 128), F32)], axis=0)
    weights = jnp.concatenate([dot(coefs[:, :P_SIZE], ratio) - coefs, ends], axis=0)
    own = dot_rows(weights, dot(b[...], weights))
    small = jnp.concatenate([own[:P_SIZE, :P_SIZE], own[P_SIZE:, P_SIZE:]], axis=1)
    keep = lax.broadcasted_iota(jnp.int32, (256, 512), 1) < count[0]
    resid = choose(panel, index[0]) - dot(jnp.where(keep, prior[...], 0.0), coefs)
    resid = resid - dot(resid[:, :P_SIZE], ratio)
    tri, inverse = factor(small)
    both = jnp.concatenate([jnp.where(on_left, inverse, 0.0), jnp.where(on_left, 0.0, inverse)], axis=0)
    basis[...] = scale * lax.dot_general(
        resid, both, (((1,), (1,)), ((), ())), precision=lax.Precision.HIGHEST, preferred_element_type=F32
    )
    tri_one = jnp.where(on_left, tri, 0.0)
    factors[0:512, :] = coefs
    factors[512:576, :] = tri_one + dot(tri_one[:, :P_SIZE], ratio)
    factors[576:640, :] = jnp.where(on_left, 0.0, tri)


def project(scale, count, index, gram, plain, prior, panel):
    return pl.pallas_call(
        functools.partial(project_kernel, scale),
        out_shape=(jax.ShapeDtypeStruct((256, 128), F32), jax.ShapeDtypeStruct((640, 128), F32)),
        in_specs=[pl.BlockSpec(memory_space=pltpu.SMEM)] * 2 + [vmem()] * 4,
        out_specs=(vmem(),) * 2,
        scratch_shapes=[pltpu.VMEM((640, 640), F32)] * 2,
        compiler_params=pltpu.CompilerParams(vmem_limit_bytes=16 * 1024 * 1024),
        name="project",
    )(count, index, gram, plain, prior, panel)


def shards(sketch, prior_basis, panel_block, panel_index, prior_count):
    far = [pltpu.with_memory_space_constraint(v, pltpu.MemorySpace.HBM) for v in (sketch, prior_basis, panel_block)]
    gram, plain = sketch_gram(prior_count, panel_index, *far)
    scale = math.sqrt(prior_basis.shape[0] * 256)
    return project(scale, prior_count, panel_index, gram, plain, prior_basis, panel_block)


def solution(mesh):
    torus = Mesh(mesh.devices.reshape(4, 8, 4, 2), AXES)
    return jax.shard_map(
        shards,
        mesh=torus,
        in_specs=(P(None, AXES), P(AXES, None), P(AXES, None), P(), P()),
        out_specs=(P(AXES, None), P()),
        check_vma=False,
    )
```

```python
import functools
import math

import jax
import jax.numpy as jnp
from jax import lax
from jax.experimental import pallas as pl
from jax.experimental.pallas import tpu as pltpu
from jax.sharding import Mesh
from jax.sharding import PartitionSpec as P

P_SIZE = 64
AXES = ("x", "z", "y", "c")
MESH = pl.DeviceIdType.MESH
F32 = jnp.float32
BF16 = jnp.bfloat16


def vmem():
    return pl.BlockSpec(memory_space=pltpu.VMEM)


def dot(left, right):
    return jnp.dot(left, right, precision=lax.Precision.HIGHEST, preferred_element_type=F32)


def thirds(value):
    high = value.astype(BF16)
    rest = value - high.astype(F32)
    middle = rest.astype(BF16)
    return high, middle, (rest - middle.astype(F32)).astype(BF16)


def deep(left, right, rows=False):
    lh, lm, ll = thirds(left)
    rh, rm, rl = thirds(right)
    axis = 0 if rows else 1
    dims = (((axis,), (0,)), ((), ()))
    value = None
    for pair, other in (((lh, ll), (rl, rh)), ((lh, lm), (rm, rh)), ((lh, lm), (rh, rm))):
        term = lax.dot_general(
            jnp.concatenate(pair, axis=axis), jnp.concatenate(other, axis=0), dims, preferred_element_type=F32
        )
        value = term if value is None else value + term
    return value


def dot_rows(left, right):
    return lax.dot_general(
        left, right, (((0,), (0,)), ((), ())), precision=lax.Precision.HIGHEST, preferred_element_type=F32
    )


def split(value):
    high = value.astype(BF16)
    return high, (value - high.astype(F32)).astype(BF16)


def halves(place):
    first = (place + 1) - 2 * lax.rem(place, 2)
    second = lax.rem(place + 3 + 2 * lax.rem(place, 2), 4)
    return (first, lax.rem((place + 1) // 2, 2)), (second, place // 2)


def square(part_high, part_low, lo):
    value = None
    for left in (part_low, part_high):
        for right in (part_low, part_high):
            term = lax.dot_general(
                left[:, lo:lo + 128], right[:, lo:], (((0,), (0,)), ((), ())), preferred_element_type=F32
            )
            value = term if value is None else value + term
    return value


def choose(panel, index):
    return jnp.where(
        index == 0, panel[:, 0:128], jnp.where(index == 1, panel[:, 64:192], panel[:, 128:256])
    )


ARRIVALS = (0, 1, 7, 2, 6, 3, 5, 4)
BLOCKS = [(i, j) for i in range(5) for j in range(i, 5)]
TILE = (8, 768)
NEAREST_FIRST = (1, 7, 2, 6, 3, 5, 4)


def gram_kernel(count, index, sketch_hbm, prior_hbm, panel_hbm, out, plain, sketch, prior, panel, high, low, dense, away, came, acc,
                r0, r1, r2, zout, zin, zall, full, mine, other, load,
                d_send, d_recv, r_send, r_recv, z_send, z_recv, y_send, y_recv, a_send, a_recv, m_send, m_recv, b_send, b_recv):
    loads = [pltpu.make_async_copy(prior_hbm, prior, load.at[0]), pltpu.make_async_copy(panel_hbm, panel, load.at[1])]
    for i in range(8):
        rows = pl.ds(256 * i, 256)
        loads.append(pltpu.make_async_copy(sketch_hbm.at[rows], sketch.at[rows], load.at[2 + i]))
    for copy in loads:
        copy.start()

    x, z, y, c = (lax.axis_index(name) for name in AXES)
    (xa, xa_bit), (xb, xb_bit) = halves(x)
    (ya, ya_bit), (yb, yb_bit) = halves(y)
    bits = (xa_bit, ya_bit, xb_bit, yb_bit)
    links = ({"x": xa}, {"y": ya}, {"x": xb}, {"y": yb})
    ring = [{"z": lax.rem(z + step, 8)} for step in range(1, 8)]
    peer = {"c": 1 - c}

    barrier = pltpu.get_barrier_semaphore()
    corners = [{**links[i], **links[(i + 1) % 4]} for i in range(4)]
    for target in [peer] + list(links) + corners + ring:
        pl.semaphore_signal(barrier, inc=1, device_id=target, device_id_type=MESH)

    def remote(source, target, send, recv, device):
        return pltpu.make_async_remote_copy(
            src_ref=source, dst_ref=target, send_sem=send, recv_sem=recv, device_id=device, device_id_type=MESH
        )

    def kept(s, t, bits=bits):
        return sum([bits[(s + u) % 4] * (8 >> u) for u in range(t)], jnp.int32(0))

    def gone(s, t, bits=bits):
        return kept(s, t, bits) + (1 - bits[(s + t) % 4]) * (8 >> t)

    turned_bits, turned_links = [], []
    for turn in range(4):
        link = lax.rem(z + turn, 4)
        upper, odd = link // 2, lax.rem(link, 2)

        def pick(values):
            return (1 - upper) * ((1 - odd) * values[0] + odd * values[1]) + upper * (
                (1 - odd) * values[2] + odd * values[3]
            )

        turned_bits.append(pick(bits))
        turned_links.append({"x": pick((xa, x, xb, x)), "y": pick((y, ya, y, yb))})

    for copy in loads[:2]:
        copy.wait()
    keep = lax.broadcasted_iota(jnp.int32, (256, 512), 1) < count[0]
    high[:, :512], low[:, :512] = split(jnp.where(keep, prior[...], 0.0))
    high[:, 512:], low[:, 512:] = split(choose(panel, index[0]))
    for i in range(5):
        lo = 128 * i
        value = square(high, low, lo)
        for j in range(i, 5):
            at = 128 * (j - i)
            dense[BLOCKS.index((i, j))] = value[:, at:at + 128].reshape(16, 8, 128)
    dense[15] = jnp.zeros((16, 8, 128), F32)
    for copy in loads[2:]:
        copy.wait()

    def product(core, tiles, target):
        rows = [sketch[pl.ds(pl.multiple_of(core * 1024 + s * 128 + tiles[s] * 8, 64), 64), :] for s in range(8)]
        part_high, part_low = split(jnp.concatenate(rows, axis=0))
        value = jnp.dot(part_high, low[...], preferred_element_type=F32)
        value = value + jnp.dot(part_low, high[...], preferred_element_type=F32)
        value = value + jnp.dot(part_high, high[...], preferred_element_type=F32)
        for s in range(8):
            target[s, pl.ds(tiles[s], 8), :, :640] = value[64 * s:64 * s + 64].reshape(8, 8, 640)
            target[s, pl.ds(tiles[s], 8), :, 640:] = dense[core * 8 + s, pl.ds(tiles[s], 8)]

    parts = ([gone(s, 0) for s in range(8)], [kept(s, 1) for s in range(8)])

    def chunk(part, s):
        tile = parts[part][s]
        return remote(
            away.at[s, pl.ds(tile, 8)], came.at[s, pl.ds(tile, 8)], d_send.at[part, s], d_recv.at[part, s], peer
        )

    for part in range(2):
        product(1 - c, parts[part], away)
    pl.semaphore_wait(barrier, 16)
    for part in range(2):
        for s in range(8):
            chunk(part, s).start()
    for part in range(2):
        product(c, parts[part], acc)

    landing = (r0, r1)

    def scatter(t, s):
        size = 8 >> t
        return remote(
            acc.at[s, pl.ds(gone(s, t), size)], landing[t].at[s], r_send.at[t, s], r_recv.at[t, s],
            links[(s + t) % 4],
        )

    def corner(s, slot):
        over, up = bits[(s + 2) % 4], bits[(s + 3) % 4]
        over = over if slot == 1 else 1 - over
        up = up if slot == 0 else 1 - up
        device = (links[(s + 2) % 4], links[(s + 3) % 4], corners[(s + 2) % 4])[slot]
        return remote(
            acc.at[s, pl.ds(kept(s, 2) + 2 * over + up, 1)], r2.at[s, pl.ds(slot, 1)],
            r_send.at[2 + slot, s], r_recv.at[2 + slot, s], device,
        )

    def along(s):
        return remote(zout.at[s], zin.at[z], z_send.at[s], z_recv.at[z], {"z": jnp.int32(s)})

    for part in range(2):
        for s in range(8):
            chunk(part, s).wait_recv()
            acc[s, pl.ds(parts[part][s], 8)] += came[s, pl.ds(parts[part][s], 8)]
            if part == 0:
                scatter(0, s).start()
    for t in range(2):
        size = 8 >> t
        for s in range(8):
            scatter(t, s).wait_recv()
            acc[s, pl.ds(kept(s, t + 1), size)] += landing[t][s]
            if t == 0:
                scatter(1, s).start()
            else:
                for slot in (2, 0, 1):
                    corner(s, slot).start()
    for s in range(8):
        for slot in range(3):
            corner(s, slot).wait_recv()
        zout[s] = acc[s, kept(s, 4)] + (r2[s, 0] + r2[s, 1] + r2[s, 2])

        @pl.when(z != s)
        def _():
            along(s).start()

    total = zout[z]
    for step in range(1, 8):
        source = lax.rem(z + step, 8)
        remote(zout.at[0], zin.at[source], z_send.at[0], z_recv.at[source], ring[0]).wait_recv()
        total = total + zin[source]
    zall[0] = total

    def back(step):
        return remote(zall.at[0], zall.at[8 - step], y_send.at[step - 1], y_recv.at[step - 1], ring[step - 1])

    for step in NEAREST_FIRST:
        back(step).start()

    def gather(t, s):
        here = full.at[s, pl.ds(kept(s, t + 1, turned_bits), 8 >> t)]
        return remote(here, here, a_send.at[t, s], a_recv.at[t, s], turned_links[(s + t) % 4])

    def gather_corner(s, slot):
        one, two = turned_links[(s + 2) % 4], turned_links[(s + 3) % 4]
        device = (one, two, {"x": one["x"] + two["x"] - x, "y": one["y"] + two["y"] - y})[slot]
        here = full.at[s, pl.ds(kept(s, 4, turned_bits), 1)]
        return remote(zall.at[pl.ds(s, 1)], here, a_send.at[2 + slot, s], a_recv.at[2 + slot, s], device)

    for s in ARRIVALS:
        if s:
            back(8 - s).wait_recv()
        for slot in (2, 0, 1):
            gather_corner(s, slot).start()
        full[s, pl.ds(kept(s, 4, turned_bits), 1)] = zall[pl.ds(s, 1)]
    for s in ARRIVALS:
        for slot in range(3):
            gather_corner(s, slot).wait_recv()
        gather(1, s).start()
    for s in ARRIVALS:
        gather(1, s).wait_recv()
        gather(0, s).start()

    def swap(i):
        lo = 128 * i
        place = (pl.ds(lo, 128), pl.ds(lo, 640 - lo))
        return remote(mine.at[place], other.at[place], m_send.at[i], m_recv.at[i], peer)

    ours = pl.ds(8 * c, 8)
    trade = remote(plain.at[ours], plain.at[ours], b_send, b_recv, peer)

    def add_gram(rows, first, last):
        part_high, part_low = split(rows)
        for i in range(5):
            lo = 128 * i
            value = square(part_high, part_low, lo)
            if first:
                mine[lo:lo + 128, lo:] = value
            else:
                mine[lo:lo + 128, lo:] += value
            if last:
                swap(i).start()

    def part_of(s, at):
        return full[s, pl.ds(at, 8), :, :640].reshape(64, 640)

    add_gram(jnp.concatenate([part_of(s, kept(s, 1, turned_bits)) for s in range(8)], axis=0), True, False)
    for last, some in ((False, ARRIVALS[:4]), (True, ARRIVALS[4:])):
        rows = []
        for s in some:
            gather(0, s).wait_recv()
            rows.append(part_of(s, gone(s, 0, turned_bits)))
            plain[8 * c + lax.rem(z + s, 8)] = full[s, :, :, 640:]
        if last:
            trade.start()
        add_gram(jnp.concatenate(rows, axis=0), False, last)
    for i in range(5):
        lo = 128 * i
        swap(i).wait_recv()
        out[lo:lo + 128, lo:] = mine[lo:lo + 128, lo:] + other[lo:lo + 128, lo:]
    trade.wait_recv()

    for s in range(8):
        for part in range(2):
            chunk(part, s).wait_send()
        for t in range(2):
            scatter(t, s).wait_send()
            gather(t, s).wait_send()
        for slot in range(3):
            corner(s, slot).wait_send()
            gather_corner(s, slot).wait_send()

        @pl.when(z != s)
        def _():
            along(s).wait_send()

    for step in range(1, 8):
        back(step).wait_send()
    for i in range(5):
        swap(i).wait_send()
    trade.wait_send()


def sketch_gram(count, index, sketch, prior, panel):
    dma = pltpu.SemaphoreType.DMA
    stream = (8, 16) + TILE
    scratch = [pltpu.VMEM((2048, 256), F32), pltpu.VMEM((256, 512), F32), pltpu.VMEM((256, 256), F32)]
    scratch += [pltpu.VMEM((256, 640), BF16)] * 2 + [pltpu.VMEM((16, 16, 8, 128), F32)]
    scratch += [pltpu.VMEM(stream, F32)] * 3
    scratch += [pltpu.VMEM((8, size) + TILE, F32) for size in (8, 4, 3)]
    scratch += [pltpu.VMEM((8,) + TILE, F32)] * 3
    scratch += [pltpu.VMEM(stream, F32)]
    scratch += [pltpu.VMEM((640, 640), F32)] * 2
    scratch += [dma((10,))] + [dma((2, 8))] * 2 + [dma((5, 8))] * 2
    scratch += [dma((8,))] * 2 + [dma((7,))] * 2 + [dma((5, 8))] * 2 + [dma((5,))] * 2 + [dma] * 2
    smem = pl.BlockSpec(memory_space=pltpu.SMEM)
    hbm = pl.BlockSpec(memory_space=pltpu.MemorySpace.HBM)
    return pl.pallas_call(
        gram_kernel,
        out_shape=(jax.ShapeDtypeStruct((640, 640), F32), jax.ShapeDtypeStruct((16, 16, 8, 128), F32)),
        in_specs=[smem, smem, hbm, hbm, hbm],
        out_specs=(vmem(),) * 2,
        scratch_shapes=scratch,
        compiler_params=pltpu.CompilerParams(
            collective_id=0, has_side_effects=True, vmem_limit_bytes=50 * 1024 * 1024
        ),
        name="sketch_gram",
    )(count, index, sketch, prior, panel)


def sweep(blocks, first):
    panels = len(blocks)
    blocks = list(blocks)
    lane = lax.broadcasted_iota(jnp.int32, (8, 128), 1)
    row = lax.broadcasted_iota(jnp.int32, (8, 128), 0)

    def columns(block, k):
        return [jnp.broadcast_to(block[:, k + s:k + s + 1], (8, 128)) for s in range(8)]

    e = columns(blocks[0], first)
    for p in range(panels):
        k = first + 8 * p
        inside = (lane >= k) & (lane < k + 8)
        cols = [columns(b, k) if i != p else None for i, b in enumerate(blocks)]
        r = jnp.where(inside, (lane - k == row).astype(F32), blocks[p])
        more = p + 1 < panels
        after = columns(blocks[p], k + 8) if more else []
        following = columns(blocks[p + 1], k + 8) if more else []
        for s in range(8):
            here = row == s
            inv = 1.0 / e[s][s:s + 1, :]

            def step(v):
                own = v[s:s + 1, :] * inv
                return jnp.where(here, own, v - e[s] * own)

            for u in range(s + 1, 8):
                e[u] = step(e[u])
            after = [step(v) for v in after]
            r = step(r)
        if more:
            e = []
            for u in range(8):
                terms = [cols[p + 1][s] * after[u][s:s + 1, :] for s in range(8)]
                while len(terms) > 1:
                    terms = [x + y for x, y in zip(terms[::2], terms[1::2])]
                e.append(following[u] - terms[0])
        for i in range(len(blocks)):
            if i == p:
                continue
            total = jnp.where(inside, 0.0, blocks[i])
            for s in range(8):
                total = total - cols[i][s] * r[s:s + 1, :]
            blocks[i] = total
        blocks[p] = r
    return blocks


def eliminated(rows, first):
    return jnp.concatenate(sweep([rows[8 * i:8 * i + 8] for i in range(8)], first), axis=0)


def inverse_of(block):
    on_left = lax.broadcasted_iota(jnp.int32, (64, 128), 1) < P_SIZE
    top = eliminated(block[:64], 0)
    bottom = jnp.where(on_left, 0.0, block[64:]) - dot(block[64:, :64], top)
    bottom = eliminated(bottom, 64)
    top = jnp.where(on_left, top, 0.0) - dot(top[:, 64:], bottom)
    return jnp.concatenate([top, bottom], axis=0)


def factor(small):
    lane = lax.broadcasted_iota(jnp.int32, (8, 128), 1)
    row = lax.broadcasted_iota(jnp.int32, (8, 128), 0)
    left = lane < P_SIZE
    place = jnp.where(left, lane, lane - P_SIZE)
    blocks = [small[8 * i:8 * i + 8, :] for i in range(8)]
    extra = [(place == row + 8 * i).astype(F32) for i in range(8)]
    roots, inverses = [], []
    for p in range(8):
        k = 8 * p

        def column(block, s):
            first = jnp.broadcast_to(block[:, k + s:k + s + 1], (8, 128))
            second = jnp.broadcast_to(block[:, P_SIZE + k + s:P_SIZE + k + s + 1], (8, 128))
            return jnp.where(left, first, second)

        cols = {i: [column(blocks[i], s) for s in range(8)] for i in range(p, 8)}
        e = list(cols[p])
        r, q = blocks[p], extra[p]
        for s in range(8):
            pivot = e[s][s:s + 1, :]
            inv = 1.0 / pivot
            root = lax.rsqrt(pivot)
            roots.append(jnp.where(place[:1] >= k + s, r[s:s + 1, :] * root, 0.0))
            inverses.append(q[s:s + 1, :] * root)
            rs, qs = r[s:s + 1, :] * inv, q[s:s + 1, :] * inv
            here = row == s
            r = jnp.where(here, rs, r - e[s] * rs)
            q = jnp.where(here, qs, q - e[s] * qs)
            for u in range(s + 1, 8):
                es = e[u][s:s + 1, :] * inv
                e[u] = jnp.where(here, es, e[u] - e[s] * es)
        for i in range(p + 1, 8):
            for s in range(8):
                blocks[i] = blocks[i] - cols[i][s] * r[s:s + 1, :]
                extra[i] = extra[i] - cols[i][s] * q[s:s + 1, :]
    return jnp.concatenate(roots, axis=0), jnp.concatenate(inverses, axis=0)


def project_kernel(scale, count, index, gram, plain, prior, panel, basis, factors, a, b):
    r = lax.broadcasted_iota(jnp.int32, (128, 128), 0)
    c = lax.broadcasted_iota(jnp.int32, (128, 128), 1)
    on_left = lax.broadcasted_iota(jnp.int32, (64, 128), 1) < P_SIZE
    for at, (i, j) in enumerate(BLOCKS):
        block = plain[at].reshape(128, 128)
        b[128 * i:128 * i + 128, 128 * j:128 * j + 128] = block
        if i != j:
            b[128 * j:128 * j + 128, 128 * i:128 * i + 128] = block.T
    for i in range(5):
        a[128 * i:128 * i + 128, 128 * i:] = gram[128 * i:128 * i + 128, 128 * i:]
    for k in range(4):
        lo = 128 * k
        hi = lo + 128
        unused = (c + lo >= count[0]) & (r == c)
        block = a[lo:hi, lo:hi] + jnp.where(unused, 1.0, 0.0)
        y = deep(inverse_of(block), a[lo:hi, hi:])
        for i in range(k + 1, 5):
            left = 128 * i
            a[left:left + 128, left:] -= deep(a[lo:hi, left:left + 128], y[:, left - hi:], True)
        if k:
            a[:lo, hi:] -= deep(a[:lo, lo:hi], y)
        a[lo:hi, hi:] = y
    coefs = a[:512, 512:]
    keep = lax.broadcasted_iota(jnp.int32, (256, 512), 1) < count[0]
    resid = choose(panel, index[0]) - dot(jnp.where(keep, prior[...], 0.0), coefs)
    weights = jnp.concatenate([-coefs, (r == c).astype(F32)], axis=0)
    own = dot_rows(weights, dot(b[...], weights))
    both = eliminated(a[512:576, 512:], 0)
    ratio = jnp.where(on_left, 0.0, both)
    own = own - dot(own[:, :P_SIZE], ratio)
    own = own - dot_rows(ratio, own[:P_SIZE])
    small = jnp.concatenate([own[:P_SIZE, :P_SIZE], own[P_SIZE:, P_SIZE:]], axis=1)
    resid = resid - dot(resid[:, :P_SIZE], ratio)
    tri, inverse = factor(small)
    both = jnp.concatenate([jnp.where(on_left, inverse, 0.0), jnp.where(on_left, 0.0, inverse)], axis=0)
    basis[...] = scale * lax.dot_general(
        resid, both, (((1,), (1,)), ((), ())), precision=lax.Precision.HIGHEST, preferred_element_type=F32
    )
    tri_one = jnp.where(on_left, tri, 0.0)
    factors[0:512, :] = coefs
    factors[512:576, :] = tri_one + dot(tri_one[:, :P_SIZE], ratio)
    factors[576:640, :] = jnp.where(on_left, 0.0, tri)


def project(scale, count, index, gram, plain, prior, panel):
    return pl.pallas_call(
        functools.partial(project_kernel, scale),
        out_shape=(jax.ShapeDtypeStruct((256, 128), F32), jax.ShapeDtypeStruct((640, 128), F32)),
        in_specs=[pl.BlockSpec(memory_space=pltpu.SMEM)] * 2 + [vmem()] * 4,
        out_specs=(vmem(),) * 2,
        scratch_shapes=[pltpu.VMEM((640, 640), F32)] * 2,
        compiler_params=pltpu.CompilerParams(vmem_limit_bytes=16 * 1024 * 1024),
        name="project",
    )(count, index, gram, plain, prior, panel)


def shards(sketch, prior_basis, panel_block, panel_index, prior_count):
    far = [pltpu.with_memory_space_constraint(v, pltpu.MemorySpace.HBM) for v in (sketch, prior_basis, panel_block)]
    gram, plain = sketch_gram(prior_count, panel_index, *far)
    scale = math.sqrt(prior_basis.shape[0] * 256)
    return project(scale, prior_count, panel_index, gram, plain, prior_basis, panel_block)


def solution(mesh):
    torus = Mesh(mesh.devices.reshape(4, 8, 4, 2), AXES)
    return jax.shard_map(
        shards,
        mesh=torus,
        in_specs=(P(None, AXES), P(AXES, None), P(AXES, None), P(), P()),
        out_specs=(P(AXES, None), P()),
        check_vma=False,
    )
```

```python
import functools
import math

import jax
import jax.numpy as jnp
from jax import lax
from jax.experimental import pallas as pl
from jax.experimental.pallas import tpu as pltpu
from jax.sharding import Mesh
from jax.sharding import PartitionSpec as P

P_SIZE = 64
AXES = ("x", "z", "y", "c")
MESH = pl.DeviceIdType.MESH
F32 = jnp.float32
BF16 = jnp.bfloat16


def vmem():
    return pl.BlockSpec(memory_space=pltpu.VMEM)


def dot(left, right):
    return jnp.dot(left, right, precision=lax.Precision.HIGHEST, preferred_element_type=F32)


def thirds(value):
    high = value.astype(BF16)
    rest = value - high.astype(F32)
    middle = rest.astype(BF16)
    return high, middle, (rest - middle.astype(F32)).astype(BF16)


def deep(left, right, rows=False):
    lh, lm, ll = thirds(left)
    rh, rm, rl = thirds(right)
    axis = 0 if rows else 1
    dims = (((axis,), (0,)), ((), ()))
    value = None
    for pair, other in (((lh, ll), (rl, rh)), ((lh, lm), (rm, rh)), ((lh, lm), (rh, rm))):
        term = lax.dot_general(
            jnp.concatenate(pair, axis=axis), jnp.concatenate(other, axis=0), dims, preferred_element_type=F32
        )
        value = term if value is None else value + term
    return value


def dot_rows(left, right):
    return lax.dot_general(
        left, right, (((0,), (0,)), ((), ())), precision=lax.Precision.HIGHEST, preferred_element_type=F32
    )


def split(value):
    high = value.astype(BF16)
    return high, (value - high.astype(F32)).astype(BF16)


def halves(place):
    first = (place + 1) - 2 * lax.rem(place, 2)
    second = lax.rem(place + 3 + 2 * lax.rem(place, 2), 4)
    return (first, lax.rem((place + 1) // 2, 2)), (second, place // 2)


def square(part_high, part_low, lo):
    value = None
    for left in (part_low, part_high):
        for right in (part_low, part_high):
            term = lax.dot_general(
                left[:, lo:lo + 128], right[:, lo:], (((0,), (0,)), ((), ())), preferred_element_type=F32
            )
            value = term if value is None else value + term
    return value


def choose(panel, index):
    return jnp.where(
        index == 0, panel[:, 0:128], jnp.where(index == 1, panel[:, 64:192], panel[:, 128:256])
    )


ARRIVALS = (0, 1, 7, 2, 6, 3, 5, 4)
BLOCKS = [(i, j) for i in range(5) for j in range(i, 5)]
TILE = (8, 768)
NEAREST_FIRST = (1, 7, 2, 6, 3, 5, 4)


def gram_kernel(count, index, sketch_hbm, prior_hbm, panel_hbm, out, plain, sketch, prior, panel, high, low, dense, away, came, acc,
                r0, r1, r2, zout, zin, zall, full, mine, other, load,
                d_send, d_recv, r_send, r_recv, z_send, z_recv, y_send, y_recv, a_send, a_recv, m_send, m_recv, b_send, b_recv):
    loads = [pltpu.make_async_copy(prior_hbm, prior, load.at[0]), pltpu.make_async_copy(panel_hbm, panel, load.at[1])]
    for i in range(8):
        rows = pl.ds(256 * i, 256)
        loads.append(pltpu.make_async_copy(sketch_hbm.at[rows], sketch.at[rows], load.at[2 + i]))
    for copy in loads:
        copy.start()

    x, z, y, c = (lax.axis_index(name) for name in AXES)
    (xa, xa_bit), (xb, xb_bit) = halves(x)
    (ya, ya_bit), (yb, yb_bit) = halves(y)
    bits = (xa_bit, ya_bit, xb_bit, yb_bit)
    links = ({"x": xa}, {"y": ya}, {"x": xb}, {"y": yb})
    ring = [{"z": lax.rem(z + step, 8)} for step in range(1, 8)]
    peer = {"c": 1 - c}

    barrier = pltpu.get_barrier_semaphore()
    corners = [{**links[i], **links[(i + 1) % 4]} for i in range(4)]
    for target in [peer] + list(links) + corners + ring:
        pl.semaphore_signal(barrier, inc=1, device_id=target, device_id_type=MESH)

    def remote(source, target, send, recv, device):
        return pltpu.make_async_remote_copy(
            src_ref=source, dst_ref=target, send_sem=send, recv_sem=recv, device_id=device, device_id_type=MESH
        )

    def kept(s, t, bits=bits):
        return sum([bits[(s + u) % 4] * (8 >> u) for u in range(t)], jnp.int32(0))

    def gone(s, t, bits=bits):
        return kept(s, t, bits) + (1 - bits[(s + t) % 4]) * (8 >> t)

    turned_bits, turned_links = [], []
    for turn in range(4):
        link = lax.rem(z + turn, 4)
        upper, odd = link // 2, lax.rem(link, 2)

        def pick(values):
            return (1 - upper) * ((1 - odd) * values[0] + odd * values[1]) + upper * (
                (1 - odd) * values[2] + odd * values[3]
            )

        turned_bits.append(pick(bits))
        turned_links.append({"x": pick((xa, x, xb, x)), "y": pick((y, ya, y, yb))})

    for copy in loads[:2]:
        copy.wait()
    keep = lax.broadcasted_iota(jnp.int32, (256, 512), 1) < count[0]
    high[:, :512], low[:, :512] = split(jnp.where(keep, prior[...], 0.0))
    high[:, 512:], low[:, 512:] = split(choose(panel, index[0]))
    for i in range(5):
        lo = 128 * i
        value = square(high, low, lo)
        for j in range(i, 5):
            at = 128 * (j - i)
            dense[BLOCKS.index((i, j))] = value[:, at:at + 128].reshape(16, 8, 128)
    dense[15] = jnp.zeros((16, 8, 128), F32)
    for copy in loads[2:]:
        copy.wait()

    def product(core, tiles, target):
        rows = [sketch[pl.ds(pl.multiple_of(core * 1024 + s * 128 + tiles[s] * 8, 64), 64), :] for s in range(8)]
        part_high, part_low = split(jnp.concatenate(rows, axis=0))
        value = jnp.dot(part_high, low[...], preferred_element_type=F32)
        value = value + jnp.dot(part_low, high[...], preferred_element_type=F32)
        value = value + jnp.dot(part_high, high[...], preferred_element_type=F32)
        for s in range(8):
            target[s, pl.ds(tiles[s], 8), :, :640] = value[64 * s:64 * s + 64].reshape(8, 8, 640)
            target[s, pl.ds(tiles[s], 8), :, 640:] = dense[core * 8 + s, pl.ds(tiles[s], 8)]

    parts = ([gone(s, 0) for s in range(8)], [kept(s, 1) for s in range(8)])

    def chunk(part, s):
        tile = parts[part][s]
        return remote(
            away.at[s, pl.ds(tile, 8)], came.at[s, pl.ds(tile, 8)], d_send.at[part, s], d_recv.at[part, s], peer
        )

    for part in range(2):
        product(1 - c, parts[part], away)
    pl.semaphore_wait(barrier, 16)
    for part in range(2):
        for s in range(8):
            chunk(part, s).start()
    for part in range(2):
        product(c, parts[part], acc)

    landing = (r0, r1)

    def scatter(t, s):
        size = 8 >> t
        return remote(
            acc.at[s, pl.ds(gone(s, t), size)], landing[t].at[s], r_send.at[t, s], r_recv.at[t, s],
            links[(s + t) % 4],
        )

    def corner(s, slot):
        over, up = bits[(s + 2) % 4], bits[(s + 3) % 4]
        over = over if slot == 1 else 1 - over
        up = up if slot == 0 else 1 - up
        device = (links[(s + 2) % 4], links[(s + 3) % 4], corners[(s + 2) % 4])[slot]
        return remote(
            acc.at[s, pl.ds(kept(s, 2) + 2 * over + up, 1)], r2.at[s, pl.ds(slot, 1)],
            r_send.at[2 + slot, s], r_recv.at[2 + slot, s], device,
        )

    def along(s):
        return remote(zout.at[s], zin.at[z], z_send.at[s], z_recv.at[z], {"z": jnp.int32(s)})

    for part in range(2):
        for s in range(8):
            chunk(part, s).wait_recv()
            acc[s, pl.ds(parts[part][s], 8)] += came[s, pl.ds(parts[part][s], 8)]
            if part == 0:
                scatter(0, s).start()
    for t in range(2):
        size = 8 >> t
        for s in range(8):
            scatter(t, s).wait_recv()
            acc[s, pl.ds(kept(s, t + 1), size)] += landing[t][s]
            if t == 0:
                scatter(1, s).start()
            else:
                for slot in (2, 0, 1):
                    corner(s, slot).start()
    for s in range(8):
        for slot in range(3):
            corner(s, slot).wait_recv()
        zout[s] = acc[s, kept(s, 4)] + (r2[s, 0] + r2[s, 1] + r2[s, 2])

        @pl.when(z != s)
        def _():
            along(s).start()

    total = zout[z]
    for step in range(1, 8):
        source = lax.rem(z + step, 8)
        remote(zout.at[0], zin.at[source], z_send.at[0], z_recv.at[source], ring[0]).wait_recv()
        total = total + zin[source]
    zall[0] = total

    def back(step):
        return remote(zall.at[0], zall.at[8 - step], y_send.at[step - 1], y_recv.at[step - 1], ring[step - 1])

    for step in NEAREST_FIRST:
        back(step).start()

    def gather(t, s):
        here = full.at[s, pl.ds(kept(s, t + 1, turned_bits), 8 >> t)]
        return remote(here, here, a_send.at[t, s], a_recv.at[t, s], turned_links[(s + t) % 4])

    def gather_corner(s, slot):
        one, two = turned_links[(s + 2) % 4], turned_links[(s + 3) % 4]
        device = (one, two, {"x": one["x"] + two["x"] - x, "y": one["y"] + two["y"] - y})[slot]
        here = full.at[s, pl.ds(kept(s, 4, turned_bits), 1)]
        return remote(zall.at[pl.ds(s, 1)], here, a_send.at[2 + slot, s], a_recv.at[2 + slot, s], device)

    for s in ARRIVALS:
        if s:
            back(8 - s).wait_recv()
        for slot in (2, 0, 1):
            gather_corner(s, slot).start()
        full[s, pl.ds(kept(s, 4, turned_bits), 1)] = zall[pl.ds(s, 1)]
    for s in ARRIVALS:
        for slot in range(3):
            gather_corner(s, slot).wait_recv()
        gather(1, s).start()
    for s in ARRIVALS:
        gather(1, s).wait_recv()
        gather(0, s).start()

    def swap(i):
        lo = 128 * i
        place = (pl.ds(lo, 128), pl.ds(lo, 640 - lo))
        return remote(mine.at[place], other.at[place], m_send.at[i], m_recv.at[i], peer)

    ours = pl.ds(8 * c, 8)
    trade = remote(plain.at[ours], plain.at[ours], b_send, b_recv, peer)

    def add_gram(rows, first, last):
        part_high, part_low = split(rows)
        for i in range(5):
            lo = 128 * i
            value = square(part_high, part_low, lo)
            if first:
                mine[lo:lo + 128, lo:] = value
            else:
                mine[lo:lo + 128, lo:] += value
            if last:
                swap(i).start()

    def part_of(s, at):
        return full[s, pl.ds(at, 8), :, :640].reshape(64, 640)

    add_gram(jnp.concatenate([part_of(s, kept(s, 1, turned_bits)) for s in range(8)], axis=0), True, False)
    for last, some in ((False, ARRIVALS[:4]), (True, ARRIVALS[4:])):
        rows = []
        for s in some:
            gather(0, s).wait_recv()
            rows.append(part_of(s, gone(s, 0, turned_bits)))
            plain[8 * c + lax.rem(z + s, 8)] = full[s, :, :, 640:]
        if last:
            trade.start()
        add_gram(jnp.concatenate(rows, axis=0), False, last)
    for i in range(5):
        lo = 128 * i
        swap(i).wait_recv()
        out[lo:lo + 128, lo:] = mine[lo:lo + 128, lo:] + other[lo:lo + 128, lo:]
    trade.wait_recv()

    for s in range(8):
        for part in range(2):
            chunk(part, s).wait_send()
        for t in range(2):
            scatter(t, s).wait_send()
            gather(t, s).wait_send()
        for slot in range(3):
            corner(s, slot).wait_send()
            gather_corner(s, slot).wait_send()

        @pl.when(z != s)
        def _():
            along(s).wait_send()

    for step in range(1, 8):
        back(step).wait_send()
    for i in range(5):
        swap(i).wait_send()
    trade.wait_send()


def sketch_gram(count, index, sketch, prior, panel):
    dma = pltpu.SemaphoreType.DMA
    stream = (8, 16) + TILE
    scratch = [pltpu.VMEM((2048, 256), F32), pltpu.VMEM((256, 512), F32), pltpu.VMEM((256, 256), F32)]
    scratch += [pltpu.VMEM((256, 640), BF16)] * 2 + [pltpu.VMEM((16, 16, 8, 128), F32)]
    scratch += [pltpu.VMEM(stream, F32)] * 3
    scratch += [pltpu.VMEM((8, size) + TILE, F32) for size in (8, 4, 3)]
    scratch += [pltpu.VMEM((8,) + TILE, F32)] * 3
    scratch += [pltpu.VMEM(stream, F32)]
    scratch += [pltpu.VMEM((640, 640), F32)] * 2
    scratch += [dma((10,))] + [dma((2, 8))] * 2 + [dma((5, 8))] * 2
    scratch += [dma((8,))] * 2 + [dma((7,))] * 2 + [dma((5, 8))] * 2 + [dma((5,))] * 2 + [dma] * 2
    smem = pl.BlockSpec(memory_space=pltpu.SMEM)
    hbm = pl.BlockSpec(memory_space=pltpu.MemorySpace.HBM)
    return pl.pallas_call(
        gram_kernel,
        out_shape=(jax.ShapeDtypeStruct((640, 640), F32), jax.ShapeDtypeStruct((16, 16, 8, 128), F32)),
        in_specs=[smem, smem, hbm, hbm, hbm],
        out_specs=(vmem(),) * 2,
        scratch_shapes=scratch,
        compiler_params=pltpu.CompilerParams(
            collective_id=0, has_side_effects=True, vmem_limit_bytes=50 * 1024 * 1024
        ),
        name="sketch_gram",
    )(count, index, sketch, prior, panel)


def sweep(blocks, first):
    panels = len(blocks)
    blocks = list(blocks)
    lane = lax.broadcasted_iota(jnp.int32, (8, 128), 1)
    row = lax.broadcasted_iota(jnp.int32, (8, 128), 0)

    def columns(block, k):
        return [jnp.broadcast_to(block[:, k + s:k + s + 1], (8, 128)) for s in range(8)]

    e = columns(blocks[0], first)
    for p in range(panels):
        k = first + 8 * p
        inside = (lane >= k) & (lane < k + 8)
        cols = [columns(b, k) if i != p else None for i, b in enumerate(blocks)]
        r = jnp.where(inside, (lane - k == row).astype(F32), blocks[p])
        more = p + 1 < panels
        after = columns(blocks[p], k + 8) if more else []
        following = columns(blocks[p + 1], k + 8) if more else []
        for s in range(8):
            here = row == s
            inv = 1.0 / e[s][s:s + 1, :]

            def step(v):
                own = v[s:s + 1, :] * inv
                return jnp.where(here, own, v - e[s] * own)

            for u in range(s + 1, 8):
                e[u] = step(e[u])
            after = [step(v) for v in after]
            r = step(r)
        if more:
            e = []
            for u in range(8):
                terms = [cols[p + 1][s] * after[u][s:s + 1, :] for s in range(8)]
                while len(terms) > 1:
                    terms = [x + y for x, y in zip(terms[::2], terms[1::2])]
                e.append(following[u] - terms[0])
        for i in range(len(blocks)):
            if i == p:
                continue
            total = jnp.where(inside, 0.0, blocks[i])
            for s in range(8):
                total = total - cols[i][s] * r[s:s + 1, :]
            blocks[i] = total
        blocks[p] = r
    return blocks


def eliminated(rows, first):
    return jnp.concatenate(sweep([rows[8 * i:8 * i + 8] for i in range(8)], first), axis=0)


def inverse_of(block):
    on_left = lax.broadcasted_iota(jnp.int32, (64, 128), 1) < P_SIZE
    top = eliminated(block[:64], 0)
    none = jnp.zeros((64, 128), F32)
    bottom = jnp.where(on_left, 0.0, block[64:])
    bottom = bottom - deep(block[64:] - bottom, jnp.concatenate([top, none], axis=0))
    bottom = eliminated(bottom, 64)
    kept = jnp.where(on_left, top, 0.0)
    top = kept - deep(top - kept, jnp.concatenate([none, bottom], axis=0))
    return jnp.concatenate([top, bottom], axis=0)


def factor(small):
    lane = lax.broadcasted_iota(jnp.int32, (8, 128), 1)
    row = lax.broadcasted_iota(jnp.int32, (8, 128), 0)
    left = lane < P_SIZE
    place = jnp.where(left, lane, lane - P_SIZE)
    blocks = [small[8 * i:8 * i + 8, :] for i in range(8)]
    extra = [(place == row + 8 * i).astype(F32) for i in range(8)]
    roots, inverses = [], []
    for p in range(8):
        k = 8 * p

        def column(block, s):
            first = jnp.broadcast_to(block[:, k + s:k + s + 1], (8, 128))
            second = jnp.broadcast_to(block[:, P_SIZE + k + s:P_SIZE + k + s + 1], (8, 128))
            return jnp.where(left, first, second)

        cols = {i: [column(blocks[i], s) for s in range(8)] for i in range(p, 8)}
        e = list(cols[p])
        r, q = blocks[p], extra[p]
        for s in range(8):
            pivot = e[s][s:s + 1, :]
            inv = 1.0 / pivot
            root = lax.rsqrt(pivot)
            roots.append(jnp.where(place[:1] >= k + s, r[s:s + 1, :] * root, 0.0))
            inverses.append(q[s:s + 1, :] * root)
            rs, qs = r[s:s + 1, :] * inv, q[s:s + 1, :] * inv
            here = row == s
            r = jnp.where(here, rs, r - e[s] * rs)
            q = jnp.where(here, qs, q - e[s] * qs)
            for u in range(s + 1, 8):
                es = e[u][s:s + 1, :] * inv
                e[u] = jnp.where(here, es, e[u] - e[s] * es)
        for i in range(p + 1, 8):
            for s in range(8):
                blocks[i] = blocks[i] - cols[i][s] * r[s:s + 1, :]
                extra[i] = extra[i] - cols[i][s] * q[s:s + 1, :]
    return jnp.concatenate(roots, axis=0), jnp.concatenate(inverses, axis=0)


def project_kernel(scale, count, index, gram, plain, prior, panel, basis, factors, a, b):
    r = lax.broadcasted_iota(jnp.int32, (128, 128), 0)
    c = lax.broadcasted_iota(jnp.int32, (128, 128), 1)
    on_left = lax.broadcasted_iota(jnp.int32, (64, 128), 1) < P_SIZE
    for at, (i, j) in enumerate(BLOCKS):
        block = plain[at].reshape(128, 128)
        b[128 * i:128 * i + 128, 128 * j:128 * j + 128] = block
        if i != j:
            b[128 * j:128 * j + 128, 128 * i:128 * i + 128] = block.T
    for i in range(5):
        a[128 * i:128 * i + 128, 128 * i:] = gram[128 * i:128 * i + 128, 128 * i:]
    for k in range(4):
        lo = 128 * k
        hi = lo + 128
        unused = (c + lo >= count[0]) & (r == c)
        block = a[lo:hi, lo:hi] + jnp.where(unused, 1.0, 0.0)
        y = deep(inverse_of(block), a[lo:hi, hi:])
        for i in range(k + 1, 5):
            left = 128 * i
            a[left:left + 128, left:] -= deep(a[lo:hi, left:left + 128], y[:, left - hi:], True)
        if k:
            a[:lo, hi:] -= deep(a[:lo, lo:hi], y)
        a[lo:hi, hi:] = y
    coefs = a[:512, 512:]
    keep = lax.broadcasted_iota(jnp.int32, (256, 512), 1) < count[0]
    resid = choose(panel, index[0]) - dot(jnp.where(keep, prior[...], 0.0), coefs)
    weights = jnp.concatenate([-coefs, (r == c).astype(F32)], axis=0)
    own = dot_rows(weights, dot(b[...], weights))
    both = eliminated(a[512:576, 512:], 0)
    ratio = jnp.where(on_left, 0.0, both)
    own = own - dot(own[:, :P_SIZE], ratio)
    own = own - dot_rows(ratio, own[:P_SIZE])
    small = jnp.concatenate([own[:P_SIZE, :P_SIZE], own[P_SIZE:, P_SIZE:]], axis=1)
    resid = resid - dot(resid[:, :P_SIZE], ratio)
    tri, inverse = factor(small)
    both = jnp.concatenate([jnp.where(on_left, inverse, 0.0), jnp.where(on_left, 0.0, inverse)], axis=0)
    basis[...] = scale * lax.dot_general(
        resid, both, (((1,), (1,)), ((), ())), precision=lax.Precision.HIGHEST, preferred_element_type=F32
    )
    tri_one = jnp.where(on_left, tri, 0.0)
    factors[0:512, :] = coefs
    factors[512:576, :] = tri_one + dot(tri_one[:, :P_SIZE], ratio)
    factors[576:640, :] = jnp.where(on_left, 0.0, tri)


def project(scale, count, index, gram, plain, prior, panel):
    return pl.pallas_call(
        functools.partial(project_kernel, scale),
        out_shape=(jax.ShapeDtypeStruct((256, 128), F32), jax.ShapeDtypeStruct((640, 128), F32)),
        in_specs=[pl.BlockSpec(memory_space=pltpu.SMEM)] * 2 + [vmem()] * 4,
        out_specs=(vmem(),) * 2,
        scratch_shapes=[pltpu.VMEM((640, 640), F32)] * 2,
        compiler_params=pltpu.CompilerParams(vmem_limit_bytes=16 * 1024 * 1024),
        name="project",
    )(count, index, gram, plain, prior, panel)


def shards(sketch, prior_basis, panel_block, panel_index, prior_count):
    far = [pltpu.with_memory_space_constraint(v, pltpu.MemorySpace.HBM) for v in (sketch, prior_basis, panel_block)]
    gram, plain = sketch_gram(prior_count, panel_index, *far)
    scale = math.sqrt(prior_basis.shape[0] * 256)
    return project(scale, prior_count, panel_index, gram, plain, prior_basis, panel_block)


def solution(mesh):
    torus = Mesh(mesh.devices.reshape(4, 8, 4, 2), AXES)
    return jax.shard_map(
        shards,
        mesh=torus,
        in_specs=(P(None, AXES), P(AXES, None), P(AXES, None), P(), P()),
        out_specs=(P(AXES, None), P()),
        check_vma=False,
    )
```
